512 devices in a mesh: env: 16 (over z), cand: 32 (over y, x, core).
Axes of the slice: x: 4, y: 4, z: 16, core: 2. Of those that a mesh axis runs over, the one named last changes fastest.
Arguments:
- white: bfloat16 [3, 256, 256, 4096], P(None, 'env', 'cand'), may hold values from -5 to 5
- mean_init: float32 [256, 2560], P('env'), may hold values from -0.3 to 0.3
- std_init: float32 [256, 2560], P('env'), may hold values from 0.05 to 0.8
- init_state: float32 [256, 128], P('env'), may hold values from -3 to 3
- goal_state: float32 [256, 128], P('env'), may hold values from -3 to 3
- w_state: bfloat16 [128, 512], replicated, may hold values from -0.5 to 0.5
- w_action: bfloat16 [64, 512], replicated, may hold values from -1.5 to 1.5
- w_out: bfloat16 [512, 128], replicated, may hold values from -0.25 to 0.25
- bias_in: float32 [512], replicated, may hold values from -3 to 3
- bias_out: float32 [128], replicated, may hold values from -3 to 3
- elite_idx: int32 [256, 3, 25], P('env'), may hold values from 0 to 255, all different within a row
Outputs:
- final_mean: float32 [256, 2560], P('env')
- final_std: float32 [256, 2560], P('env')
- costs: float32 [3, 256, 256], P(None, 'env', 'cand')
The draws below stay inside these ranges and needn't reach their ends.
Inputs may be any that keep to these rules, and one draw needn't show every extreme that they name: `elite_idx`: each row names 25 different candidates.
All inputs are finite; a program needn't handle non-finite values.
Results may differ from the reference program's by a relative error of at most 0.0031.
Values sent between devices are 32-bit elements; how exact they have to be, the bound alone decides.
No kernel may reach another device: no remote copies, remote signals or barrier semaphores. Data moves between devices by JAX's collectives and lax.ppermute only.
A program may use at most 128 MiB of HBM per device.

```python
import math
import jax
import jax.numpy as jnp
from jax import lax

ENV_DEV = 16
ITERS = 3
HORIZON = 40
NOISE_LEN = 64
ACT = 64
STATE = 128
HIDDEN_SIZE = 512
ENVS = 256
CAND = 256
ELITES = 25


def steps_of(rng, shape, cuts, least, largest):
    factor_of, own = 1.0, jax.random.fold_in(rng, 6)
    for dim, shards_of in cuts:
        steps = jnp.exp(jax.random.uniform(jax.random.fold_in(own, dim), (shards_of,), jnp.float32, least / len(cuts), largest / len(cuts)))
        factor_of = factor_of * jnp.repeat(steps, shape[dim] // shards_of).reshape([-1 if axis == dim else 1 for axis in range(len(shape))])
    return factor_of


def choose_distinct(own_key, rows, number_of, top, lift):
    ranking = jax.random.permutation(jax.random.fold_in(own_key, 1), number_of)
    boost = ranking
    for power in range(3):
        boost = boost * boost // number_of
    boost = boost * lift // number_of
    tickets = jax.random.randint(jax.random.fold_in(own_key, 2), (rows, number_of), 0, 4096) + boost
    sure = jax.random.permutation(jax.random.fold_in(own_key, 3), rows)[jnp.arange(number_of) % rows]
    tickets = jnp.where(jnp.arange(rows)[:, None] == sure[None, :], 1 << 14, tickets)
    merit = tickets * number_of + jnp.arange(number_of)
    return lax.top_k(merit.astype(jnp.int32), top)[1].astype(jnp.int32)


def bell_draw(stream_key, dims, deviation, most, cuts=(), kind=jnp.bfloat16):
    array = deviation * jax.random.normal(stream_key, dims, jnp.float32)
    if cuts:
        array = array * steps_of(stream_key, dims, cuts, -0.22, 0.18)
    return jnp.clip(array, -most, most).astype(kind)


def setup_inputs(seed: int = 0) -> dict:
    keys = jax.random.split(jax.random.key(seed), 12)
    white = bell_draw(keys[0], (ITERS, ENVS, CAND, NOISE_LEN * ACT), 1.0, 5.0, ((1, 16), (2, 32)))
    mean_init = jnp.clip(jax.random.uniform(keys[1], (ENVS, HORIZON * ACT), jnp.float32, -0.3, 0.3) * steps_of(keys[1], (ENVS, HORIZON * ACT), ((0, 16),), -0.4, 0.0), -0.3, 0.3)
    std_init = jnp.clip(jnp.exp(math.log(0.8) - 2.7725887 * jax.random.uniform(keys[2], (ENVS, HORIZON * ACT), jnp.float32) ** steps_of(keys[2], (ENVS, HORIZON * ACT), ((0, 16),), -0.2, 0.2)), 0.05, 0.8)
    init_state = bell_draw(keys[3], (ENVS, STATE), 0.5, 3.0, ((0, 16),), jnp.float32)
    goal_state = bell_draw(keys[4], (ENVS, STATE), 0.5, 3.0, ((0, 16),), jnp.float32)
    w_state = bell_draw(keys[5], (STATE, HIDDEN_SIZE), STATE ** -0.5, 0.5)
    w_action = bell_draw(keys[6], (ACT, HIDDEN_SIZE), (ACT // 4) ** -0.5, 1.5)
    w_out = bell_draw(keys[7], (HIDDEN_SIZE, STATE), HIDDEN_SIZE ** -0.5, 0.25)
    bias_in = bell_draw(keys[8], (HIDDEN_SIZE,), 0.5, 3.0, (), jnp.float32)
    bias_out = bell_draw(keys[9], (STATE,), 0.5, 3.0, (), jnp.float32)
    elite_idx = choose_distinct(keys[10], ENVS * ITERS, CAND, ELITES, 0).reshape((ENVS, ITERS, ELITES))
    return dict(white=white, mean_init=mean_init, std_init=std_init, init_state=init_state, goal_state=goal_state, w_state=w_state, w_action=w_action, w_out=w_out, bias_in=bias_in, bias_out=bias_out, elite_idx=elite_idx)


BETA_EXP = 2.5
MOMENTUM = 0.1
FLOOR_SHARE = 0.1
ACT_COST = 0.1

def colored_ref(white_block):
    env_count, cand_count, flat = white_block.shape
    series = white_block.astype(jnp.float32).reshape(env_count, cand_count, NOISE_LEN, ACT)
    freqs = jnp.arange(NOISE_LEN // 2 + 1, dtype=jnp.int32)
    scale = (jnp.maximum(freqs, 1).astype(jnp.float32) / NOISE_LEN) ** (-BETA_EXP / 2)
    kernel = jnp.fft.irfft(scale, n=NOISE_LEN)
    kernel = kernel / jnp.sqrt(jnp.sum(kernel * kernel))
    kernel_low = lax.optimization_barrier(kernel.astype(jnp.bfloat16))
    kernel_back = kernel_low.astype(jnp.float32)
    kernel_freq = jnp.fft.rfft(kernel_back, n=NOISE_LEN)
    spectrum = jnp.fft.rfft(series, axis=2) * kernel_freq[None, None, :, None]
    colored = jnp.fft.irfft(spectrum, n=NOISE_LEN, axis=2)[:, :, :HORIZON, :]
    return colored.reshape(env_count, cand_count, HORIZON * ACT).astype(jnp.float32)

def rollout(actions, start, goal, w_state, w_action, w_out, bias_in, bias_out):
    ordered = jnp.swapaxes(actions, 0, 1)

    def advance(state, action):
        pre = jnp.dot(state.astype(jnp.bfloat16), w_state, preferred_element_type=jnp.float32)
        pre = pre + jnp.dot(action.astype(jnp.bfloat16), w_action, preferred_element_type=jnp.float32) + bias_in
        hidden = jax.nn.silu(pre).astype(jnp.bfloat16)
        state = jnp.tanh(state + jnp.dot(hidden, w_out, preferred_element_type=jnp.float32) + bias_out)
        error = state - goal
        step_cost = lax.optimization_barrier(jnp.mean(error * error, axis=-1)) + ACT_COST * lax.optimization_barrier(jnp.mean(action * action, axis=-1))
        return (state, step_cost)
    final, step_costs = lax.scan(advance, start, ordered)
    return lax.optimization_barrier(jnp.mean(step_costs, axis=0))

def reference(white, mean_init, std_init, init_state, goal_state, w_state, w_action, w_out, bias_in, bias_out, elite_idx):
    blocks = ENVS // ENV_DEV
    center, spread = (mean_init, std_init)
    cost_list = []
    for iteration in range(ITERS):

        def block_work(pieces):
            white_block, center_block, spread_block, start_block, goal_block, elite_block = pieces
            noise = colored_ref(white_block)
            actions = jnp.clip(center_block[:, None, :] + spread_block[:, None, :] * noise, -1.0, 1.0)
            rows = ENV_DEV * CAND
            starts = jnp.broadcast_to(start_block[:, None, :], (ENV_DEV, CAND, STATE)).reshape(rows, STATE)
            goals = jnp.broadcast_to(goal_block[:, None, :], (ENV_DEV, CAND, STATE)).reshape(rows, STATE)
            block_costs = rollout(actions.reshape(rows, HORIZON, ACT), starts, goals, w_state, w_action, w_out, bias_in, bias_out)
            member = lax.optimization_barrier(jnp.sum((elite_block[:, :, None] == jnp.arange(CAND, dtype=jnp.int32)[None, None, :]).astype(jnp.float32), axis=1))
            sums = jnp.einsum('ec,ech->eh', member, actions, precision=lax.Precision.HIGHEST)
            squares = jnp.einsum('ec,ech->eh', member, actions * actions, precision=lax.Precision.HIGHEST)
            return (block_costs.reshape(ENV_DEV, CAND), sums, squares)
        pieces = (white[iteration].reshape(blocks, ENV_DEV, CAND, NOISE_LEN * ACT), center.reshape(blocks, ENV_DEV, HORIZON * ACT), spread.reshape(blocks, ENV_DEV, HORIZON * ACT), init_state.reshape(blocks, ENV_DEV, STATE), goal_state.reshape(blocks, ENV_DEV, STATE), elite_idx[:, iteration, :].reshape(blocks, ENV_DEV, ELITES))
        block_costs, sums, squares = lax.map(block_work, pieces)
        cost_list.append(block_costs.reshape(ENVS, CAND))
        sums = sums.reshape(ENVS, HORIZON * ACT)
        squares = squares.reshape(ENVS, HORIZON * ACT)
        elite_mean = sums / ELITES
        variance = jnp.maximum(squares / ELITES - elite_mean * elite_mean, 0.0)
        center = MOMENTUM * center + (1.0 - MOMENTUM) * elite_mean
        mixed = MOMENTUM * spread + (1.0 - MOMENTUM) * jnp.sqrt(variance)
        env_peak = lax.optimization_barrier(jnp.max(mixed, axis=1))
        peak = jnp.max(env_peak)
        settled = jnp.mean(env_peak / peak)
        spread = jnp.maximum(mixed, FLOOR_SHARE * peak) * (0.5 + settled)
    return (center, spread, jnp.stack(cost_list))
```

```python
import functools

import jax
import jax.numpy as jnp
import numpy as np
from jax import lax
from jax.experimental import pallas as pl
from jax.experimental.pallas import tpu as pltpu
from jax.sharding import PartitionSpec as P

BETA_EXP = 2.5
MOMENTUM = 0.1
FLOOR_SHARE = 0.1
ACT_COST = 0.1
LANES = 128
VMEM = pl.BlockSpec(memory_space=pltpu.VMEM)
SMEM = pl.BlockSpec(memory_space=pltpu.SMEM)


def color_kernel(length):
    freqs = np.arange(length // 2 + 1)
    scale = (np.maximum(freqs, 1).astype(np.float32) / np.float32(length)) ** np.float32(-BETA_EXP / 2)
    kernel = np.fft.irfft(scale.astype(np.float64), n=length)
    kernel = kernel / np.sqrt(np.sum(kernel * kernel))
    return np.asarray(kernel, np.float32).astype(jnp.bfloat16).astype(np.float32)


def band_rows(length, act_dim):
    per = 256 // act_dim
    kernel = color_kernel(length)
    rows = np.arange(length)[:, None]
    quarter = np.arange(256)[None, :] // act_dim
    return jnp.asarray(kernel[(quarter - rows) % length], jnp.float32), per


def noise_body(white_ref, band_ref, out_ref, fill, *, act_dim, blocks):
    length = band_ref.shape[0]
    flat = length * act_dim

    @pl.when(pl.program_id(0) == 0)
    def _():
        row = lax.broadcasted_iota(jnp.int32, (act_dim, 256), 0)
        lane = lax.broadcasted_iota(jnp.int32, (act_dim, 256), 1)
        hit = lane % act_dim == row
        for j in range(length):
            tile = jnp.where(hit, band_ref[pl.ds(j, 1), :], 0.0).astype(jnp.bfloat16)
            fill[pl.ds(j * act_dim, act_dim), :] = tile
            fill[pl.ds(flat + j * act_dim, act_dim), :] = tile

    for block in range(blocks):
        start = (flat - block * 256) % flat
        out_ref[0, :, pl.ds(block * 256, 256)] = jnp.dot(
            white_ref[0], fill[pl.ds(start, flat), :], preferred_element_type=jnp.float32
        )


def noise_of(white, first, count, band, act_dim, horizon):
    _, rows, flat = white.shape
    width = horizon * act_dim
    return pl.pallas_call(
        functools.partial(noise_body, act_dim=act_dim, blocks=width // 256),
        grid=(count,),
        in_specs=[
            pl.BlockSpec((1, rows, flat), lambda i: (i + first, 0, 0)),
            pl.BlockSpec(band.shape, lambda i: (0, 0)),
        ],
        out_specs=pl.BlockSpec((1, rows, width), lambda i: (i, 0, 0)),
        out_shape=jax.ShapeDtypeStruct((count, rows, width), jnp.float32),
        scratch_shapes=[pltpu.VMEM((2 * flat, 256), jnp.bfloat16)],
        compiler_params=pltpu.CompilerParams(vmem_limit_bytes=40 << 20),
        name="noise",
    )(white, band)


def action_body(*refs, first, envs_total, groups):
    noise_ref, member_ref, mine_ref, state_ref, acts_ref, asq_ref, sums_ref, own_ref = refs
    half = sums_ref.shape[2]
    rows = acts_ref.shape[0]
    envs = sums_ref.shape[0] // 2
    cands = rows // envs
    me = mine_ref[0]
    if first:
        floor, gain = None, None
    else:
        peaks = state_ref[:, 0, pl.ds(half, LANES)]
        pair = jnp.max(peaks.reshape(envs, 2, LANES), axis=1)
        peak = jnp.max(pair, axis=(0, 1), keepdims=True)
        total = jnp.sum(jnp.sum(pair, axis=0, keepdims=True), axis=1, keepdims=True)
        floor = FLOOR_SHARE * peak
        gain = 0.5 + total / (peak * envs_total)

    def spread_of(mixed):
        return mixed if first else jnp.maximum(mixed, floor) * gain

    own = state_ref[me, :, pl.ds(0, half)]
    own_ref[0:1, :] = own[0:1]
    own_ref[1:2, :] = spread_of(own[1:2])
    for env in range(envs):
        at = pl.ds(env * cands, cands)
        member = member_ref[at, :]
        square = jnp.zeros((cands, LANES), jnp.float32)
        for side in range(2):
            line = 2 * env + side
            for step in range(half // LANES):
                lanes = pl.ds(step * LANES, LANES)
                whole = pl.ds(side * half + step * LANES, LANES)
                center = state_ref[line, 0:1, lanes]
                spread = spread_of(state_ref[line, 1:2, lanes])
                action = jnp.clip(center + spread * noise_ref[0, at, whole], -1.0, 1.0)
                acts_ref[at, whole] = action.astype(jnp.bfloat16)
                both = action * action
                square = square + both
                sums_ref[line, 0:1, lanes] = jnp.sum(action * member, axis=0, keepdims=True)
                sums_ref[line, 1:2, lanes] = jnp.sum(both * member, axis=0, keepdims=True)
        asq_ref[at, :] = square


def actions_of(noise, at, member, mine, state, first, envs_total, groups, lines, half):
    _, rows, width = noise.shape
    return pl.pallas_call(
        functools.partial(action_body, first=first, envs_total=envs_total, groups=groups),
        grid=(1,),
        in_specs=[
            pl.BlockSpec((1, rows, width), lambda i: (at, 0, 0)),
            VMEM,
            SMEM,
            VMEM,
        ],
        out_specs=[VMEM, VMEM, VMEM, VMEM],
        out_shape=[
            jax.ShapeDtypeStruct((rows, width), jnp.bfloat16),
            jax.ShapeDtypeStruct((rows, LANES), jnp.float32),
            jax.ShapeDtypeStruct((lines, 2, half), jnp.float32),
            jax.ShapeDtypeStruct((2, half), jnp.float32),
        ],
        name="actions",
    )(noise, member, mine, state)


def refit_body(parts_ref, own_ref, slice_ref, peak_ref, *, elites):
    total = jnp.sum(parts_ref[...], axis=0)
    mean = total[0:1] / elites
    variance = jnp.maximum(total[1:2] / elites - mean * mean, 0.0)
    slice_ref[0:1, :] = MOMENTUM * own_ref[0:1, :] + (1.0 - MOMENTUM) * mean
    mixed = MOMENTUM * own_ref[1:2, :] + (1.0 - MOMENTUM) * jnp.sqrt(variance)
    slice_ref[1:2, :] = mixed
    peak_ref[...] = jnp.broadcast_to(jnp.max(mixed, axis=1, keepdims=True)[None], peak_ref.shape)


def refit(parts, own, elites, groups):
    return pl.pallas_call(
        functools.partial(refit_body, elites=elites),
        in_specs=[VMEM, VMEM],
        out_specs=[VMEM, VMEM],
        out_shape=[
            jax.ShapeDtypeStruct(own.shape, jnp.float32),
            jax.ShapeDtypeStruct((groups, 1, LANES), jnp.float32),
        ],
        name="refit",
    )(parts, own)


def spread_body(slice_ref, peak_ref, out_ref):
    lines, _, wide = out_ref.shape
    half = slice_ref.shape[1]
    lane = lax.broadcasted_iota(jnp.int32, (1, LANES), 1)
    tail = jnp.zeros((1, LANES), jnp.float32)
    for group in range(peak_ref.shape[0]):
        tail = jnp.where(lane == group, peak_ref[group], tail)
    main = jnp.broadcast_to(slice_ref[...][None], (lines, 2, half))
    out_ref[:, :, pl.ds(0, half)] = main
    out_ref[:, :, pl.ds(half, LANES)] = jnp.broadcast_to(tail[None], (lines, 2, LANES))


def to_all(piece, peaks, lines):
    half = piece.shape[1]
    return pl.pallas_call(
        spread_body,
        in_specs=[VMEM, VMEM],
        out_specs=VMEM,
        out_shape=jax.ShapeDtypeStruct((lines, 2, half + LANES), jnp.float32),
        name="to_all",
    )(piece, peaks)


def final_body(state_ref, mean_ref, std_ref, *, envs_total):
    envs, width = mean_ref.shape
    half = width // 2
    peaks = state_ref[:, 0, pl.ds(half, LANES)]
    pair = jnp.max(peaks.reshape(envs, 2, LANES), axis=1)
    peak = jnp.max(pair, axis=(0, 1), keepdims=True)
    total = jnp.sum(jnp.sum(pair, axis=0, keepdims=True), axis=1, keepdims=True)
    floor = FLOOR_SHARE * peak
    gain = 0.5 + total / (peak * envs_total)
    for env in range(envs):
        for side in range(2):
            lanes = pl.ds(side * half, half)
            line = 2 * env + side
            mean_ref[pl.ds(env, 1), lanes] = state_ref[line, 0:1, pl.ds(0, half)]
            std_ref[pl.ds(env, 1), lanes] = (
                jnp.maximum(state_ref[line, 1:2, pl.ds(0, half)], floor) * gain
            )


def finished(state, envs, width, envs_total):
    shape = jax.ShapeDtypeStruct((envs, width), jnp.float32)
    return pl.pallas_call(
        functools.partial(final_body, envs_total=envs_total),
        in_specs=[VMEM],
        out_specs=[VMEM, VMEM],
        out_shape=[shape, shape],
        name="finished",
    )(state)


def rollout_body(
    acts_ref, asq_ref, start_ref, goal_ref, win_ref, wout_ref, bin_ref, bout_ref, cost_ref, *, act_dim, chains
):
    rows, width = acts_ref.shape
    dim = start_ref.shape[1]
    steps = width // act_dim
    size = rows // chains

    def advance(state, pair, parity, goal):
        joined = jnp.concatenate([state.astype(jnp.bfloat16), pair], axis=1)
        half = jnp.dot(joined, win_ref[parity], preferred_element_type=jnp.float32) + bin_ref[...]
        hidden = (half + half * jnp.tanh(half)).astype(jnp.bfloat16)
        moved = jnp.dot(hidden, wout_ref[...], preferred_element_type=jnp.float32)
        state = jnp.tanh(state + moved + bout_ref[...])
        error = state - goal
        return state, error * error

    def two_steps(k, carry):
        lanes = pl.ds(pl.multiple_of(k * 2 * act_dim, 2 * act_dim), 2 * act_dim)
        out = []
        for chain in range(chains):
            at = pl.ds(chain * size, size)
            state, error = carry[chain]
            pair = acts_ref[at, lanes]
            goal = goal_ref[at, :]
            for parity in range(2):
                state, more = advance(state, pair, parity, goal)
                error = error + more
            out.append((state, error))
        return tuple(out)

    init = tuple(
        (start_ref[pl.ds(c * size, size), :], jnp.zeros((size, dim), jnp.float32)) for c in range(chains)
    )
    done = lax.fori_loop(0, steps // 2, two_steps, init)
    for chain in range(chains):
        at = pl.ds(chain * size, size)
        both = done[chain][1] / (dim * steps) + asq_ref[at, :] * (ACT_COST / (act_dim * steps))
        cost_ref[at, :] = jnp.broadcast_to(jnp.sum(both, axis=1, keepdims=True), (size, LANES))


def rollout(acts, asq, starts, goals, win, wout, bias_in, bias_out, act_dim, chains=2):
    rows, width = acts.shape
    return pl.pallas_call(
        functools.partial(rollout_body, act_dim=act_dim, chains=chains),
        in_specs=[VMEM] * 8,
        out_specs=VMEM,
        out_shape=jax.ShapeDtypeStruct((rows, LANES), jnp.float32),
        name="rollout",
    )(acts, asq, starts, goals, win, wout, bias_in, bias_out)


def shards(
    white,
    mean_init,
    std_init,
    init_state,
    goal_state,
    w_state,
    w_action,
    w_out,
    bias_in,
    bias_out,
    elite_idx,
):
    iters, envs, cands, flat = white.shape
    act_dim, hidden = w_action.shape
    dim = w_state.shape[0]
    length = flat // act_dim
    width = mean_init.shape[1]
    horizon = width // act_dim
    half = width // 2
    elites = elite_idx.shape[2]
    groups = lax.axis_size("env")
    peers = lax.axis_size("cand")
    lines = 2 * envs
    envs_total = envs * groups
    rows = envs * cands
    assert lines == peers and rows % 16 == 0
    band, _ = band_rows(length, act_dim)
    mine = lax.axis_index("cand")
    cand_ids = mine * cands + jnp.arange(cands, dtype=jnp.int32)
    member = jnp.sum(
        (elite_idx[:, :, :, None] == cand_ids).astype(jnp.float32), axis=2
    )
    member = jnp.broadcast_to(
        jnp.swapaxes(member, 0, 1).reshape(iters, rows, 1), (iters, rows, LANES)
    )
    starts = jnp.broadcast_to(init_state[:, None, :], (envs, cands, dim)).reshape(rows, dim)
    goals = jnp.broadcast_to(goal_state[:, None, :], (envs, cands, dim)).reshape(rows, dim)
    zeros = jnp.zeros_like(w_action)
    win = jnp.stack(
        [
            jnp.concatenate([w_state, w_action, zeros], axis=0),
            jnp.concatenate([w_state, zeros, w_action], axis=0),
        ]
    ) * jnp.bfloat16(0.5)
    half_bias = (0.5 * bias_in)[None]
    white = white.reshape(iters, rows, flat)
    noise_first = noise_of(white, 0, 1, band, act_dim, horizon)
    noise_rest = noise_of(white, 1, iters - 1, band, act_dim, horizon)
    state = jnp.stack(
        [mean_init.reshape(lines, half), std_init.reshape(lines, half)], axis=1
    )
    mine = mine[None].astype(jnp.int32)
    cost_list = []
    for it in range(iters):
        noise, at = (noise_first, 0) if it == 0 else (noise_rest, it - 1)
        acts, asq, sums, own = actions_of(
            noise, at, member[it], mine, state, it == 0, envs_total, groups, lines, half
        )
        parts = lax.all_to_all(sums, "cand", 0, 0, tiled=True)
        cost = rollout(acts, asq, starts, goals, win, w_out, half_bias, bias_out[None], act_dim)
        cost_list.append(cost[:, 0].reshape(envs, cands))
        piece, peak = refit(parts, own, elites, groups)
        peaks = lax.all_to_all(peak, "env", 0, 0, tiled=True)
        state = lax.all_to_all(to_all(piece, peaks, lines), "cand", 0, 0, tiled=True)
    mean, std = finished(state, envs, width, envs_total)
    return (mean, std, jnp.stack(cost_list))


def solution(mesh):
    in_specs = (
        P(None, "env", "cand", None),
        P("env", None),
        P("env", None),
        P("env", None),
        P("env", None),
        P(),
        P(),
        P(),
        P(),
        P(),
        P("env", None, None),
    )
    out_specs = (P("env", None), P("env", None), P(None, "env", "cand"))
    return jax.shard_map(shards, mesh=mesh, in_specs=in_specs, out_specs=out_specs, check_vma=False)
```

```python
import functools

import jax
import jax.numpy as jnp
import numpy as np
from jax import lax
from jax.experimental import pallas as pl
from jax.experimental.pallas import tpu as pltpu
from jax.sharding import PartitionSpec as P

BETA_EXP = 2.5
MOMENTUM = 0.1
FLOOR_SHARE = 0.1
ACT_COST = 0.1
LANES = 128
ROLL_FLOPS = 1 << 28
VMEM = pl.BlockSpec(memory_space=pltpu.VMEM)
SMEM = pl.BlockSpec(memory_space=pltpu.SMEM)
ANY = pl.BlockSpec(memory_space=pl.ANY)


def color_kernel(length):
    freqs = np.arange(length // 2 + 1)
    scale = (np.maximum(freqs, 1).astype(np.float32) / np.float32(length)) ** np.float32(-BETA_EXP / 2)
    kernel = np.fft.irfft(scale.astype(np.float64), n=length)
    kernel = kernel / np.sqrt(np.sum(kernel * kernel))
    return np.asarray(kernel, np.float32).astype(jnp.bfloat16).astype(np.float32)


def band_rows(length, act_dim):
    per = 256 // act_dim
    kernel = color_kernel(length)
    rows = np.arange(length)[:, None]
    quarter = np.arange(256)[None, :] // act_dim
    return jnp.asarray(kernel[(quarter - rows) % length], jnp.float32), per


def noise_body(white_ref, band_ref, tie_ref, out_ref, fill, *, act_dim, blocks):
    length = band_ref.shape[0]
    flat = length * act_dim

    @pl.when(pl.program_id(0) == 0)
    def _():
        row = lax.broadcasted_iota(jnp.int32, (act_dim, 256), 0)
        lane = lax.broadcasted_iota(jnp.int32, (act_dim, 256), 1)
        hit = lane % act_dim == row
        for j in range(length):
            tile = jnp.where(hit, band_ref[pl.ds(j, 1), :], 0.0).astype(jnp.bfloat16)
            fill[pl.ds(j * act_dim, act_dim), :] = tile
            fill[pl.ds(flat + j * act_dim, act_dim), :] = tile

    for block in range(blocks):
        start = (flat - block * 256) % flat
        out_ref[0, :, pl.ds(block * 256, 256)] = jnp.dot(
            white_ref[0], fill[pl.ds(start, flat), :], preferred_element_type=jnp.float32
        )


def noise_of(white, first, count, band, tie, act_dim, horizon):
    _, rows, flat = white.shape
    width = horizon * act_dim
    return pl.pallas_call(
        functools.partial(noise_body, act_dim=act_dim, blocks=width // 256),
        grid=(count,),
        in_specs=[
            pl.BlockSpec((1, rows, flat), lambda i: (i + first, 0, 0)),
            pl.BlockSpec(band.shape, lambda i: (0, 0)),
            ANY,
        ],
        out_specs=pl.BlockSpec((1, rows, width), lambda i: (i, 0, 0)),
        out_shape=jax.ShapeDtypeStruct((count, rows, width), jnp.float32),
        scratch_shapes=[pltpu.VMEM((2 * flat, 256), jnp.bfloat16)],
        compiler_params=pltpu.CompilerParams(vmem_limit_bytes=16 << 20),
        name="noise",
    )(white, band, tie)


def stats_of(state_ref, envs, half, envs_total):
    peaks = state_ref[:, 0, pl.ds(half, LANES)]
    pair = jnp.max(peaks.reshape(envs, 2, LANES), axis=1)
    peak = jnp.max(pair, axis=(0, 1), keepdims=True)
    total = jnp.sum(jnp.sum(pair, axis=0, keepdims=True), axis=1, keepdims=True)
    return FLOOR_SHARE * peak, 0.5 + total / (peak * envs_total)


def action_body(*refs, it, envs_total):
    first = it == 0
    if first:
        noise_ref, elite_ref, mine_ref, mean_ref, std_ref, acts_ref, asq_ref, sums_ref, own_ref = refs
    else:
        noise_ref, elite_ref, mine_ref, state_ref, acts_ref, asq_ref, sums_ref, own_ref = refs
    half = sums_ref.shape[2]
    rows = acts_ref.shape[0]
    envs = sums_ref.shape[0] // 2
    cands = rows // envs
    me = mine_ref[0]
    if first:
        lanes = pl.ds(pl.multiple_of((me % 2) * half, LANES), half)
        own_ref[0:1, :] = mean_ref[pl.ds(me // 2, 1), lanes]
        own_ref[1:2, :] = std_ref[pl.ds(me // 2, 1), lanes]
    else:
        floor, gain = stats_of(state_ref, envs, half, envs_total)
        own = state_ref[me, :, pl.ds(0, half)]
        own_ref[0:1, :] = own[0:1]
        own_ref[1:2, :] = jnp.maximum(own[1:2], floor) * gain
    ids = me * cands + lax.broadcasted_iota(jnp.int32, (cands, 1), 0)
    for env in range(envs):
        at = pl.ds(env * cands, cands)
        chosen = elite_ref[env, it : it + 1, :] == ids
        member = jnp.sum(jnp.where(chosen, 1.0, 0.0), axis=1, keepdims=True)
        member = jnp.broadcast_to(member, (cands, LANES))
        square = jnp.zeros((cands, LANES), jnp.float32)
        for side in range(2):
            line = 2 * env + side
            for step in range(half // LANES):
                lanes = pl.ds(step * LANES, LANES)
                whole = pl.ds(side * half + step * LANES, LANES)
                if first:
                    center = mean_ref[pl.ds(env, 1), whole]
                    spread = std_ref[pl.ds(env, 1), whole]
                else:
                    center = state_ref[line, 0:1, lanes]
                    spread = jnp.maximum(state_ref[line, 1:2, lanes], floor) * gain
                action = jnp.clip(center + spread * noise_ref[0, at, whole], -1.0, 1.0)
                acts_ref[at, whole] = action.astype(jnp.bfloat16)
                both = action * action
                square = square + both
                sums_ref[line, 0:1, lanes] = jnp.sum(action * member, axis=0, keepdims=True)
                sums_ref[line, 1:2, lanes] = jnp.sum(both * member, axis=0, keepdims=True)
        asq_ref[at, :] = square


def actions_of(noise, at, elite_idx, mine, state, it, envs_total, lines, half):
    _, rows, width = noise.shape
    return pl.pallas_call(
        functools.partial(action_body, it=it, envs_total=envs_total),
        grid=(1,),
        in_specs=[pl.BlockSpec((1, rows, width), lambda i: (at, 0, 0)), VMEM, SMEM] + [VMEM] * len(state),
        out_specs=[VMEM, VMEM, VMEM, VMEM],
        out_shape=[
            jax.ShapeDtypeStruct((rows, width), jnp.bfloat16),
            jax.ShapeDtypeStruct((rows, LANES), jnp.float32),
            jax.ShapeDtypeStruct((lines, 2, half), jnp.float32),
            jax.ShapeDtypeStruct((2, half), jnp.float32),
        ],
        compiler_params=pltpu.CompilerParams(vmem_limit_bytes=12 << 20),
        name="actions",
    )(noise, elite_idx, mine, *state)


def refit_body(parts_ref, own_ref, tie_ref, slice_ref, peak_ref, *, elites):
    total = jnp.sum(parts_ref[...], axis=0)
    mean = total[0:1] / elites
    variance = jnp.maximum(total[1:2] / elites - mean * mean, 0.0)
    slice_ref[0:1, :] = MOMENTUM * own_ref[0:1, :] + (1.0 - MOMENTUM) * mean
    mixed = MOMENTUM * own_ref[1:2, :] + (1.0 - MOMENTUM) * jnp.sqrt(variance)
    slice_ref[1:2, :] = mixed
    peak_ref[...] = jnp.broadcast_to(jnp.max(mixed, axis=1, keepdims=True)[None], peak_ref.shape)


def refit(parts, own, tie, elites, groups):
    return pl.pallas_call(
        functools.partial(refit_body, elites=elites),
        in_specs=[VMEM, VMEM, ANY],
        out_specs=[VMEM, VMEM],
        out_shape=[
            jax.ShapeDtypeStruct(own.shape, jnp.float32),
            jax.ShapeDtypeStruct((groups, 1, LANES), jnp.float32),
        ],
        compiler_params=pltpu.CompilerParams(vmem_limit_bytes=4 << 20),
        name="refit",
    )(parts, own, tie)


def spread_body(slice_ref, peak_ref, tie_ref, out_ref):
    lines = out_ref.shape[0]
    half = slice_ref.shape[1]
    lane = lax.broadcasted_iota(jnp.int32, (1, LANES), 1)
    tail = jnp.zeros((1, LANES), jnp.float32)
    for group in range(peak_ref.shape[0]):
        tail = jnp.where(lane == group, peak_ref[group], tail)
    main = jnp.broadcast_to(slice_ref[...][None], (lines, 2, half))
    out_ref[:, :, pl.ds(0, half)] = main
    out_ref[:, :, pl.ds(half, LANES)] = jnp.broadcast_to(tail[None], (lines, 2, LANES))


def to_all(piece, peaks, tie, lines):
    half = piece.shape[1]
    return pl.pallas_call(
        spread_body,
        in_specs=[VMEM, VMEM, ANY],
        out_specs=VMEM,
        out_shape=jax.ShapeDtypeStruct((lines, 2, half + LANES), jnp.float32),
        compiler_params=pltpu.CompilerParams(vmem_limit_bytes=4 << 20),
        name="to_all",
    )(piece, peaks, tie)


def final_body(state_ref, mean_ref, std_ref, *, envs_total):
    envs, width = mean_ref.shape
    half = width // 2
    floor, gain = stats_of(state_ref, envs, half, envs_total)
    for env in range(envs):
        for side in range(2):
            lanes = pl.ds(side * half, half)
            line = 2 * env + side
            mean_ref[pl.ds(env, 1), lanes] = state_ref[line, 0:1, pl.ds(0, half)]
            std_ref[pl.ds(env, 1), lanes] = (
                jnp.maximum(state_ref[line, 1:2, pl.ds(0, half)], floor) * gain
            )


def finished(state, envs, width, envs_total):
    shape = jax.ShapeDtypeStruct((envs, width), jnp.float32)
    return pl.pallas_call(
        functools.partial(final_body, envs_total=envs_total),
        in_specs=[VMEM],
        out_specs=[VMEM, VMEM],
        out_shape=[shape, shape],
        compiler_params=pltpu.CompilerParams(vmem_limit_bytes=4 << 20),
        name="finished",
    )(state)


def rollout_body(*refs, act_dim, earlier):
    (acts_ref, asq_ref, begin_ref, goal_ref, ws_ref, wa_ref, wout_ref, bin_ref, bout_ref) = refs[:9]
    before = refs[9 : 9 + earlier]
    cost_ref, win, start, goal = refs[10 + earlier :]
    rows, width = acts_ref.shape
    envs, dim = begin_ref.shape
    cands = rows // envs
    steps = width // act_dim
    zeros = jnp.zeros(wa_ref.shape, jnp.bfloat16)
    for parity in range(2):
        win[parity, pl.ds(0, dim), :] = ws_ref[...] * jnp.bfloat16(0.5)
        win[parity, pl.ds(dim + parity * act_dim, act_dim), :] = wa_ref[...] * jnp.bfloat16(0.5)
        win[parity, pl.ds(dim + (1 - parity) * act_dim, act_dim), :] = zeros
    for env in range(envs):
        at = pl.ds(env * cands, cands)
        start[at, :] = jnp.broadcast_to(begin_ref[pl.ds(env, 1), :], (cands, dim))
        goal[at, :] = jnp.broadcast_to(goal_ref[pl.ds(env, 1), :], (cands, dim))
    bias_in = bin_ref[...] * 0.5

    def two_steps(k, carry):
        state, error = carry
        pair = acts_ref[:, pl.ds(pl.multiple_of(k * 2 * act_dim, 2 * act_dim), 2 * act_dim)]
        for parity in range(2):
            joined = jnp.concatenate([state.astype(jnp.bfloat16), pair], axis=1)
            half = jnp.dot(joined, win[parity], preferred_element_type=jnp.float32) + bias_in
            hidden = (half + half * jnp.tanh(half)).astype(jnp.bfloat16)
            moved = jnp.dot(hidden, wout_ref[...], preferred_element_type=jnp.float32)
            state = jnp.tanh(state + moved + bout_ref[...])
            gap = state - goal[...]
            error = error + gap * gap
        return state, error

    _, error = lax.fori_loop(0, steps // 2, two_steps, (start[...], jnp.zeros((rows, dim), jnp.float32)))
    both = error / (dim * steps) + asq_ref[...] * (ACT_COST / (act_dim * steps))
    cost = jnp.broadcast_to(jnp.sum(both, axis=1, keepdims=True), (rows, LANES))
    lane = lax.broadcasted_iota(jnp.int32, (cands, LANES), 1)
    table = jnp.zeros((cands, LANES), jnp.float32)
    for env in range(envs):
        table = jnp.where(lane == env, cost[env * cands : (env + 1) * cands], table)
    for k in range(earlier):
        cost_ref[k] = before[k][...]
    cost_ref[earlier] = table[:, :envs]


def rollout(acts, asq, fixed, before, tie, act_dim):
    rows, width = acts.shape
    envs, dim = fixed[0].shape
    cands = rows // envs
    earlier = len(before)
    return pl.pallas_call(
        functools.partial(rollout_body, act_dim=act_dim, earlier=earlier),
        in_specs=[VMEM] * (9 + earlier) + [ANY],
        out_specs=VMEM,
        out_shape=jax.ShapeDtypeStruct((1 + earlier, cands, envs), jnp.float32),
        scratch_shapes=[
            pltpu.VMEM((2, dim + 2 * act_dim, fixed[2].shape[1]), jnp.bfloat16),
            pltpu.VMEM((rows, dim), jnp.float32),
            pltpu.VMEM((rows, dim), jnp.float32),
        ],
        cost_estimate=pl.CostEstimate(
            flops=ROLL_FLOPS, bytes_accessed=2 * rows * width, transcendentals=0
        ),
        compiler_params=pltpu.CompilerParams(vmem_limit_bytes=8 << 20),
        name="rollout",
    )(acts, asq, *fixed, *before, tie)


def shards(
    white,
    mean_init,
    std_init,
    init_state,
    goal_state,
    w_state,
    w_action,
    w_out,
    bias_in,
    bias_out,
    elite_idx,
):
    iters, envs, cands, flat = white.shape
    act_dim = w_action.shape[0]
    length = flat // act_dim
    width = mean_init.shape[1]
    horizon = width // act_dim
    half = width // 2
    elites = elite_idx.shape[2]
    groups = lax.axis_size("env")
    peers = lax.axis_size("cand")
    lines = 2 * envs
    envs_total = envs * groups
    rows = envs * cands
    assert lines == peers and rows % 16 == 0
    band, _ = band_rows(length, act_dim)
    mine = lax.axis_index("cand").astype(jnp.int32)[None]
    fixed = (init_state, goal_state, w_state, w_action, w_out, bias_in[None], bias_out[None])
    white = white.reshape(iters, rows, flat)
    noise = noise_of(white, 0, 1, band, mean_init, act_dim, horizon)
    state = (mean_init, std_init)
    costs = []
    for it in range(iters):
        at = max(it - 1, 0)
        acts, asq, sums, own = actions_of(noise, at, elite_idx, mine, state, it, envs_total, lines, half)
        parts = lax.all_to_all(sums, "cand", 0, 0, tiled=True)
        if it == 0:
            noise = noise_of(white, 1, iters - 1, band, own, act_dim, horizon)
        piece, peak = refit(parts, own, noise, elites, groups)
        peaks = lax.all_to_all(peak, "env", 0, 0, tiled=True)
        last = it == iters - 1
        costs.append(rollout(acts, asq, fixed, costs if last else [], peak, act_dim))
        if not last:
            costs[-1] = costs[-1][0]
        state = (
            lax.all_to_all(to_all(piece, peaks, costs[-1], lines), "cand", 0, 0, tiled=True),
        )
    mean, std = finished(state[0], envs, width, envs_total)
    return (mean, std, jnp.swapaxes(costs[-1], 1, 2))


def solution(mesh):
    in_specs = (
        P(None, "env", "cand", None),
        P("env", None),
        P("env", None),
        P("env", None),
        P("env", None),
        P(),
        P(),
        P(),
        P(),
        P(),
        P("env", None, None),
    )
    out_specs = (P("env", None), P("env", None), P(None, "env", "cand"))
    return jax.shard_map(shards, mesh=mesh, in_specs=in_specs, out_specs=out_specs, check_vma=False)
```

```python
import functools

import jax
import jax.numpy as jnp
import numpy as np
from jax import lax
from jax.experimental import pallas as pl
from jax.experimental.pallas import tpu as pltpu
from jax.sharding import PartitionSpec as P

BETA_EXP = 2.5
MOMENTUM = 0.1
FLOOR_SHARE = 0.1
ACT_COST = 0.1
LANES = 128
ROLL_FLOPS = 1 << 28
CUT = 22
VMEM = pl.BlockSpec(memory_space=pltpu.VMEM)
SMEM = pl.BlockSpec(memory_space=pltpu.SMEM)
HBM = pl.BlockSpec(memory_space=pltpu.HBM)


def whole(shape):
    return pl.BlockSpec(shape, lambda i: (0,) * len(shape))


def stay(array):
    return pltpu.with_memory_space_constraint(array, pltpu.HBM)


def in_hbm(shape, dtype=jnp.float32):
    return pltpu.HBM(shape, dtype)


def color_kernel(length):
    freqs = np.arange(length // 2 + 1)
    scale = (np.maximum(freqs, 1).astype(np.float32) / np.float32(length)) ** np.float32(-BETA_EXP / 2)
    kernel = np.fft.irfft(scale.astype(np.float64), n=length)
    kernel = kernel / np.sqrt(np.sum(kernel * kernel))
    return np.asarray(kernel, np.float32).astype(jnp.bfloat16).astype(np.float32)


def noise_body(white_ref, tie_ref, out_ref, rows_in, fill, sems, *, act_dim, blocks, first, parts):
    count = out_ref.shape[0]
    _, rows, flat = white_ref.shape
    length = flat // act_dim
    size = rows // parts

    def fetch(one, part):
        at = pl.ds(part * size, size)
        return pltpu.make_async_copy(
            white_ref.at[first + one, at, :], rows_in.at[one, at, :], sems.at[one * parts + part]
        )

    for one in range(count):
        for part in range(parts):
            fetch(one, part).start()
    kernel = color_kernel(length)
    row = lax.broadcasted_iota(jnp.int32, (act_dim, 256), 0)
    lane = lax.broadcasted_iota(jnp.int32, (act_dim, 256), 1)
    hit = lane % act_dim == row
    quarter = lax.broadcasted_iota(jnp.int32, (1, 256), 1) // act_dim
    for j in range(length):
        band = jnp.full((1, 256), float(kernel[-j % length]), jnp.float32)
        for q in range(1, 256 // act_dim):
            band = jnp.where(quarter == q, float(kernel[(q - j) % length]), band)
        tile = jnp.where(hit, band, 0.0).astype(jnp.bfloat16)
        fill[pl.ds(j * act_dim, act_dim), :] = tile
        fill[pl.ds(flat + j * act_dim, act_dim), :] = tile
    for one in range(count):
        for part in range(parts):
            fetch(one, part).wait()
        for block in range(blocks):
            start = (flat - block * 256) % flat
            out_ref[one, :, pl.ds(block * 256, 256)] = jnp.dot(
                rows_in[one], fill[pl.ds(start, flat), :], preferred_element_type=jnp.float32
            )


def noise_of(white, first, count, tie, act_dim, horizon):
    _, rows, flat = white.shape
    width = horizon * act_dim
    parts = 1
    return pl.pallas_call(
        functools.partial(
            noise_body, act_dim=act_dim, blocks=width // 256, first=first, parts=parts
        ),
        in_specs=[HBM, HBM],
        out_specs=VMEM,
        out_shape=jax.ShapeDtypeStruct((count, rows, width), jnp.float32),
        scratch_shapes=[
            pltpu.VMEM((count, rows, flat), jnp.bfloat16),
            pltpu.VMEM((2 * flat, 256), jnp.bfloat16),
            pltpu.SemaphoreType.DMA((count * parts,)),
        ],
        cost_estimate=pl.CostEstimate(flops=ROLL_FLOPS, bytes_accessed=1 << 20, transcendentals=0),
        compiler_params=pltpu.CompilerParams(vmem_limit_bytes=16 << 20),
        name="noise",
    )(stay(white), stay(tie))


def stats_of(state_ref, envs, half, envs_total):
    peaks = state_ref[:, 0, pl.ds(half, LANES)]
    pair = jnp.max(peaks.reshape(envs, 2, LANES), axis=1)
    peak = jnp.max(pair, axis=(0, 1), keepdims=True)
    total = jnp.sum(jnp.sum(pair, axis=0, keepdims=True), axis=1, keepdims=True)
    return FLOOR_SHARE * peak, 0.5 + total / (peak * envs_total)


def action_body(*refs, it, envs_total):
    first = it == 0
    if first:
        noise_ref, elite_ref, mine_ref, tie_ref, mean_ref, std_ref = refs[:6]
    else:
        noise_ref, elite_ref, mine_ref, tie_ref, state_ref = refs[:5]
    acts_out, asq_ref, sums_ref, own_ref, acts_ref, sems = refs[-6:]
    half = sums_ref.shape[2]
    rows = acts_ref.shape[0]
    envs = sums_ref.shape[0] // 2
    cands = rows // envs
    me = mine_ref[0]
    if first:
        lanes = pl.ds(pl.multiple_of((me % 2) * half, LANES), half)
        own_ref[0:1, :] = mean_ref[pl.ds(me // 2, 1), lanes]
        own_ref[1:2, :] = std_ref[pl.ds(me // 2, 1), lanes]
    else:
        floor, gain = stats_of(state_ref, envs, half, envs_total)
        own = state_ref[me, :, pl.ds(0, half)]
        own_ref[0:1, :] = own[0:1]
        own_ref[1:2, :] = jnp.maximum(own[1:2], floor) * gain
    per = 4

    def send(part):
        at = pl.ds(part * per * cands, per * cands)
        return pltpu.make_async_copy(acts_ref.at[at, :], acts_out.at[at, :], sems.at[part])

    ids = me * cands + lax.broadcasted_iota(jnp.int32, (cands, 1), 0)
    for env in range(envs):
        at = pl.ds(env * cands, cands)
        chosen = elite_ref[it, env : env + 1, :] == ids
        member = jnp.sum(jnp.where(chosen, 1.0, 0.0), axis=1, keepdims=True)
        member = jnp.broadcast_to(member, (cands, LANES))
        square = jnp.zeros((cands, LANES), jnp.float32)
        for side in range(2):
            line = 2 * env + side
            for step in range(half // LANES):
                lanes = pl.ds(step * LANES, LANES)
                whole = pl.ds(side * half + step * LANES, LANES)
                if first:
                    center = mean_ref[pl.ds(env, 1), whole]
                    spread = std_ref[pl.ds(env, 1), whole]
                else:
                    center = state_ref[line, 0:1, lanes]
                    spread = jnp.maximum(state_ref[line, 1:2, lanes], floor) * gain
                action = jnp.clip(center + spread * noise_ref[0, at, whole], -1.0, 1.0)
                acts_ref[at, whole] = action.astype(jnp.bfloat16)
                both = action * action
                square = square + both
                sums_ref[line, 0:1, lanes] = jnp.sum(action * member, axis=0, keepdims=True)
                sums_ref[line, 1:2, lanes] = jnp.sum(both * member, axis=0, keepdims=True)
        asq_ref[at, :] = square
        if env % per == per - 1:
            send(env // per).start()
    for part in range(envs // per):
        send(part).wait()


def actions_of(noise, at, elite_idx, mine, tie, state, it, envs_total, lines, half):
    _, rows, width = noise.shape
    return pl.pallas_call(
        functools.partial(action_body, it=it, envs_total=envs_total),
        grid=(1,),
        in_specs=[pl.BlockSpec((1, rows, width), lambda i: (at, 0, 0)), VMEM, SMEM, HBM]
        + [VMEM] * len(state),
        out_specs=[HBM, whole((rows, LANES)), whole((lines, 2, half)), whole((2, half))],
        out_shape=[
            in_hbm((rows, width), jnp.bfloat16),
            in_hbm((rows, LANES)),
            in_hbm((lines, 2, half)),
            in_hbm((2, half)),
        ],
        scratch_shapes=[
            pltpu.VMEM((rows, width), jnp.bfloat16),
            pltpu.SemaphoreType.DMA((lines // 8,)),
        ],
        compiler_params=pltpu.CompilerParams(vmem_limit_bytes=12 << 20),
        name="actions",
    )(noise, elite_idx, mine, stay(tie), *state)


def refit_body(parts_ref, own_ref, tie_ref, slice_ref, peak_ref, *, elites):
    total = jnp.sum(parts_ref[...], axis=0)
    mean = total[0:1] / elites
    variance = jnp.maximum(total[1:2] / elites - mean * mean, 0.0)
    slice_ref[0:1, :] = MOMENTUM * own_ref[0:1, :] + (1.0 - MOMENTUM) * mean
    mixed = MOMENTUM * own_ref[1:2, :] + (1.0 - MOMENTUM) * jnp.sqrt(variance)
    slice_ref[1:2, :] = mixed
    peak_ref[...] = jnp.broadcast_to(jnp.max(mixed, axis=1, keepdims=True)[None], peak_ref.shape)


def refit(parts, own, tie, elites, groups):
    return pl.pallas_call(
        functools.partial(refit_body, elites=elites),
        in_specs=[VMEM, VMEM, HBM],
        out_specs=[VMEM, VMEM],
        out_shape=[
            jax.ShapeDtypeStruct(own.shape, jnp.float32),
            jax.ShapeDtypeStruct((groups, 1, LANES), jnp.float32),
        ],
        compiler_params=pltpu.CompilerParams(vmem_limit_bytes=4 << 20),
        name="refit",
    )(parts, own, stay(tie))


def spread_body(slice_ref, peak_ref, out_ref, token_ref):
    lines = out_ref.shape[0]
    half = slice_ref.shape[1]
    lane = lax.broadcasted_iota(jnp.int32, (1, LANES), 1)
    tail = jnp.zeros((1, LANES), jnp.float32)
    for group in range(peak_ref.shape[0]):
        tail = jnp.where(lane == group, peak_ref[group], tail)
    main = jnp.broadcast_to(slice_ref[...][None], (lines, 2, half))
    out_ref[:, :, pl.ds(0, half)] = main
    token_ref[...] = jnp.broadcast_to(tail, token_ref.shape)
    out_ref[:, :, pl.ds(half, LANES)] = jnp.broadcast_to(tail[None], (lines, 2, LANES))


def to_all(piece, peaks, lines):
    half = piece.shape[1]
    return pl.pallas_call(
        spread_body,
        grid=(1,),
        in_specs=[VMEM, VMEM],
        out_specs=[whole((lines, 2, half + LANES)), whole((8, LANES))],
        out_shape=[in_hbm((lines, 2, half + LANES)), in_hbm((8, LANES))],
        compiler_params=pltpu.CompilerParams(vmem_limit_bytes=4 << 20),
        name="to_all",
    )(piece, peaks)


def final_body(state_ref, mean_ref, std_ref, *, envs_total):
    envs, width = mean_ref.shape
    half = width // 2
    floor, gain = stats_of(state_ref, envs, half, envs_total)
    for env in range(envs):
        for side in range(2):
            lanes = pl.ds(side * half, half)
            line = 2 * env + side
            mean_ref[pl.ds(env, 1), lanes] = state_ref[line, 0:1, pl.ds(0, half)]
            std_ref[pl.ds(env, 1), lanes] = (
                jnp.maximum(state_ref[line, 1:2, pl.ds(0, half)], floor) * gain
            )


def finished(state, envs, width, envs_total):
    shape = jax.ShapeDtypeStruct((envs, width), jnp.float32)
    return pl.pallas_call(
        functools.partial(final_body, envs_total=envs_total),
        in_specs=[VMEM],
        out_specs=[VMEM, VMEM],
        out_shape=[shape, shape],
        compiler_params=pltpu.CompilerParams(vmem_limit_bytes=4 << 20),
        name="finished",
    )(state)


def rollout_body(*refs, spans, act_dim, total, earlier):
    refs = list(refs)
    take = lambda n: [refs.pop(0) for _ in range(n)]
    acts = take(len(spans))
    carried = [take(1)[0] if first else None for first, _ in spans]
    squares = [take(1)[0] if last == total else None for _, last in spans]
    begin_ref, goal_ref, ws_ref, wa_ref, wout_ref, bin_ref, bout_ref = take(7)
    before = take(earlier)
    take(1)
    outs = take(len(spans))
    moves, win, start, goal, sems = refs
    envs, dim = begin_ref.shape
    rows = acts[0].shape[0]
    cands = rows // envs
    steps = spans[0][1] - spans[0][0]
    copies = []
    for k, (first, last) in enumerate(spans):
        copies.append(
            pltpu.make_async_copy(
                acts[k].at[:, pl.ds(first * act_dim, steps * act_dim)],
                moves.at[pl.ds(k * rows, rows), :],
                sems.at[k],
            )
        )
        copies[k].start()
    zeros = jnp.zeros(wa_ref.shape, jnp.bfloat16)
    for parity in range(2):
        win[parity, pl.ds(0, dim), :] = ws_ref[...] * jnp.bfloat16(0.5)
        win[parity, pl.ds(dim + parity * act_dim, act_dim), :] = wa_ref[...] * jnp.bfloat16(0.5)
        win[parity, pl.ds(dim + (1 - parity) * act_dim, act_dim), :] = zeros
    for k in range(len(spans)):
        for env in range(envs):
            at = pl.ds(k * rows + env * cands, cands)
            if carried[k] is None:
                start[0, at, :] = jnp.broadcast_to(begin_ref[pl.ds(env, 1), :], (cands, dim))
            goal[at, :] = jnp.broadcast_to(goal_ref[pl.ds(env, 1), :], (cands, dim))
        at = pl.ds(k * rows, rows)
        if carried[k] is None:
            start[1, at, :] = jnp.zeros((rows, dim), jnp.float32)
        else:
            start[0, at, :] = carried[k][0]
            start[1, at, :] = carried[k][1]
    bias_in = bin_ref[...] * 0.5
    for copy in copies:
        copy.wait()

    def two_steps(k, carry):
        state, error = carry
        pair = moves[:, pl.ds(pl.multiple_of(k * 2 * act_dim, 2 * act_dim), 2 * act_dim)]
        for parity in range(2):
            joined = jnp.concatenate([state.astype(jnp.bfloat16), pair], axis=1)
            half = jnp.dot(joined, win[parity], preferred_element_type=jnp.float32) + bias_in
            hidden = (half + half * jnp.tanh(half)).astype(jnp.bfloat16)
            moved = jnp.dot(hidden, wout_ref[...], preferred_element_type=jnp.float32)
            state = jnp.tanh(state + moved + bout_ref[...])
            gap = state - goal[...]
            error = error + gap * gap
        return state, error

    state, error = lax.fori_loop(0, steps // 2, two_steps, (start[0], start[1]))
    for k, (_, last) in enumerate(spans):
        part = slice(k * rows, (k + 1) * rows)
        if last < total:
            outs[k][0] = state[part]
            outs[k][1] = error[part]
            continue
        both = error[part] / (dim * total) + squares[k][...] * (ACT_COST / (act_dim * total))
        cost = jnp.broadcast_to(jnp.sum(both, axis=1, keepdims=True), (rows, LANES))
        lane = lax.broadcasted_iota(jnp.int32, (cands, LANES), 1)
        table = jnp.zeros((cands, LANES), jnp.float32)
        for env in range(envs):
            table = jnp.where(lane == env, cost[env * cands : (env + 1) * cands], table)
        for n in range(earlier):
            outs[k][n] = before[n][0]
        outs[k][earlier] = table[:, :envs]


def rollout(parts, fixed, before, tie, act_dim):
    rows, width = parts[0][0].shape
    envs, dim = fixed[0].shape
    cands = rows // envs
    total = width // act_dim
    spans = [(p[3], p[4]) for p in parts]
    steps = spans[0][1] - spans[0][0]
    assert all(b - a == steps and a % 2 == 0 for a, b in spans) and steps % 2 == 0
    acts = [p[0] for p in parts]
    carried = [p[2] for p in parts if p[3]]
    squares = [p[1] for p in parts if p[4] == total]
    shapes = [
        (1 + len(before), cands, envs) if last == total else (2, rows, dim) for _, last in spans
    ]
    small = len(carried) + len(squares) + len(fixed) + len(before)
    return pl.pallas_call(
        functools.partial(
            rollout_body, spans=spans, act_dim=act_dim, total=total, earlier=len(before)
        ),
        grid=(1,),
        in_specs=[HBM] * len(acts) + [VMEM] * small + [HBM],
        out_specs=[whole(shape) for shape in shapes],
        out_shape=[in_hbm(shape) for shape in shapes],
        scratch_shapes=[
            pltpu.VMEM((len(parts) * rows, steps * act_dim), jnp.bfloat16),
            pltpu.VMEM((2, dim + 2 * act_dim, fixed[2].shape[1]), jnp.bfloat16),
            pltpu.VMEM((2, len(parts) * rows, dim), jnp.float32),
            pltpu.VMEM((len(parts) * rows, dim), jnp.float32),
            pltpu.SemaphoreType.DMA((len(parts),)),
        ],
        cost_estimate=pl.CostEstimate(flops=ROLL_FLOPS, bytes_accessed=1 << 20, transcendentals=0),
        compiler_params=pltpu.CompilerParams(vmem_limit_bytes=10 << 20),
        name="rollout",
    )(*map(stay, acts), *carried, *squares, *fixed, *before, stay(tie))


def shards(
    white,
    mean_init,
    std_init,
    init_state,
    goal_state,
    w_state,
    w_action,
    w_out,
    bias_in,
    bias_out,
    elite_idx,
):
    iters, envs, cands, flat = white.shape
    act_dim = w_action.shape[0]
    length = flat // act_dim
    width = mean_init.shape[1]
    horizon = width // act_dim
    half = width // 2
    elites = elite_idx.shape[2]
    groups = lax.axis_size("env")
    peers = lax.axis_size("cand")
    lines = 2 * envs
    envs_total = envs * groups
    rows = envs * cands
    assert lines == peers and rows % 16 == 0
    assert iters == 3
    mine = lax.axis_index("cand").astype(jnp.int32)[None]
    fixed = (init_state, goal_state, w_state, w_action, w_out, bias_in[None], bias_out[None])
    white = white.reshape(iters, rows, flat)
    elite_idx = jnp.swapaxes(elite_idx, 0, 1)
    mix = functools.partial(lax.all_to_all, axis_name="cand", split_axis=0, concat_axis=0, tiled=True)
    cut = min(CUT, horizon)
    acts, asq, held, costs = {}, {}, {}, {}

    def part(it, first, last):
        return (acts[it], asq[it], held.get(it), first, last)

    def play(parts, tie, before=()):
        outs = rollout([part(*p) for p in parts], fixed, before, tie, act_dim)
        for (it, _, last), out in zip(parts, outs):
            if last < horizon:
                held[it] = out
            else:
                costs[it] = out
        return outs[0]

    noise = noise_of(white, 0, 1, mine, act_dim, horizon)
    state, tie = (mean_init, std_init), mine
    for it in range(iters):
        acts[it], asq[it], sums, own = actions_of(
            noise, max(it - 1, 0), elite_idx, mine, tie, state, it, envs_total, lines, half
        )
        parts = mix(sums)
        if it == 0:
            tie = noise = noise_of(white, 1, iters - 1, own, act_dim, horizon)
        elif it == 1:
            tie = play([(0, cut, horizon)], own)
        else:
            tie = play([(1, cut, horizon), (2, 0, horizon - cut)], own)
        piece, peak = refit(parts, own, tie, elites, groups)
        peaks = lax.all_to_all(peak, "env", 0, 0, tiled=True)
        spread, token = to_all(piece, peaks, lines)
        state = (mix(spread),)
        if it < iters - 1:
            tie = play([(it, 0, cut)], token)
        else:
            tie = play([(2, horizon - cut, horizon)], token, (costs[0], costs[1]))
    mean, std = finished(state[0], envs, width, envs_total)
    return (mean, std, jnp.swapaxes(costs[iters - 1], 1, 2))


def solution(mesh):
    in_specs = (
        P(None, "env", "cand", None),
        P("env", None),
        P("env", None),
        P("env", None),
        P("env", None),
        P(),
        P(),
        P(),
        P(),
        P(),
        P("env", None, None),
    )
    out_specs = (P("env", None), P("env", None), P(None, "env", "cand"))
    return jax.shard_map(shards, mesh=mesh, in_specs=in_specs, out_specs=out_specs, check_vma=False)
```

```python
import functools

import jax
import jax.numpy as jnp
import numpy as np
from jax import lax
from jax.experimental import pallas as pl
from jax.experimental.pallas import tpu as pltpu
from jax.sharding import PartitionSpec as P

BETA_EXP = 2.5
MOMENTUM = 0.1
FLOOR_SHARE = 0.1
ACT_COST = 0.1
LANES = 128
ROLL_FLOPS = 1 << 28
VMEM = pl.BlockSpec(memory_space=pltpu.VMEM)
SMEM = pl.BlockSpec(memory_space=pltpu.SMEM)
HBM = pl.BlockSpec(memory_space=pltpu.HBM)


def whole(shape):
    return pl.BlockSpec(shape, lambda i: (0,) * len(shape))


def stay(array):
    return pltpu.with_memory_space_constraint(array, pltpu.HBM)


def in_hbm(shape, dtype=jnp.float32):
    return pltpu.HBM(shape, dtype)


def color_kernel(length):
    freqs = np.arange(length // 2 + 1)
    scale = (np.maximum(freqs, 1).astype(np.float32) / np.float32(length)) ** np.float32(-BETA_EXP / 2)
    kernel = np.fft.irfft(scale.astype(np.float64), n=length)
    kernel = kernel / np.sqrt(np.sum(kernel * kernel))
    return np.asarray(kernel, np.float32).astype(jnp.bfloat16).astype(np.float32)


def noise_body(white_ref, tie_ref, out_ref, token_ref, rows_in, fill, sems, *, act_dim, blocks, first, parts):
    count = out_ref.shape[0]
    _, rows, flat = white_ref.shape
    length = flat // act_dim
    size = rows // parts

    def fetch(one, part):
        at = pl.ds(part * size, size)
        return pltpu.make_async_copy(
            white_ref.at[first + one, at, :], rows_in.at[one, at, :], sems.at[one * parts + part]
        )

    for one in range(count):
        for part in range(parts):
            fetch(one, part).start()
    kernel = color_kernel(length)
    row = lax.broadcasted_iota(jnp.int32, (act_dim, 256), 0)
    lane = lax.broadcasted_iota(jnp.int32, (act_dim, 256), 1)
    hit = lane % act_dim == row
    quarter = lax.broadcasted_iota(jnp.int32, (1, 256), 1) // act_dim
    for j in range(length):
        band = jnp.full((1, 256), float(kernel[-j % length]), jnp.float32)
        for q in range(1, 256 // act_dim):
            band = jnp.where(quarter == q, float(kernel[(q - j) % length]), band)
        tile = jnp.where(hit, band, 0.0).astype(jnp.bfloat16)
        fill[pl.ds(j * act_dim, act_dim), :] = tile
        fill[pl.ds(flat + j * act_dim, act_dim), :] = tile
    for one in range(count):
        for part in range(parts):
            fetch(one, part).wait()
        for block in range(blocks):
            start = (flat - block * 256) % flat
            out_ref[one, :, pl.ds(block * 256, 256)] = jnp.dot(
                rows_in[one], fill[pl.ds(start, flat), :], preferred_element_type=jnp.float32
            )
    token_ref[...] = out_ref[count - 1, pl.ds(0, 8), pl.ds(0, LANES)]


def noise_of(white, first, count, tie, act_dim, horizon):
    _, rows, flat = white.shape
    width = horizon * act_dim
    parts = 1
    return pl.pallas_call(
        functools.partial(
            noise_body, act_dim=act_dim, blocks=width // 256, first=first, parts=parts
        ),
        grid=(1,),
        in_specs=[HBM, HBM],
        out_specs=[VMEM, whole((8, LANES))],
        out_shape=[
            jax.ShapeDtypeStruct((count, rows, width), jnp.float32),
            in_hbm((8, LANES)),
        ],
        scratch_shapes=[
            pltpu.VMEM((count, rows, flat), jnp.bfloat16),
            pltpu.VMEM((2 * flat, 256), jnp.bfloat16),
            pltpu.SemaphoreType.DMA((count * parts,)),
        ],
        cost_estimate=pl.CostEstimate(flops=ROLL_FLOPS, bytes_accessed=1 << 20, transcendentals=0),
        compiler_params=pltpu.CompilerParams(vmem_limit_bytes=16 << 20),
        name="noise",
    )(stay(white), stay(tie))


def stats_of(state_ref, envs, half, envs_total):
    peaks = state_ref[:, 0, pl.ds(half, LANES)]
    pair = jnp.max(peaks.reshape(envs, 2, LANES), axis=1)
    peak = jnp.max(pair, axis=(0, 1), keepdims=True)
    total = jnp.sum(jnp.sum(pair, axis=0, keepdims=True), axis=1, keepdims=True)
    return FLOOR_SHARE * peak, 0.5 + total / (peak * envs_total)


def action_body(*refs, it, envs_total):
    first = it == 0
    if first:
        noise_ref, elite_ref, mine_ref, tie_ref, mean_ref, std_ref = refs[:6]
    else:
        noise_ref, elite_ref, mine_ref, tie_ref, state_ref = refs[:5]
    acts_out, asq_out, sums_out, own_out, acts_ref, asq_ref, sums_ref, own_ref, sems = refs[-9:]
    half = sums_ref.shape[2]
    rows = acts_ref.shape[0]
    envs = sums_ref.shape[0] // 2
    cands = rows // envs
    me = mine_ref[0]
    if first:
        lanes = pl.ds(pl.multiple_of((me % 2) * half, LANES), half)
        own_ref[0:1, :] = mean_ref[pl.ds(me // 2, 1), lanes]
        own_ref[1:2, :] = std_ref[pl.ds(me // 2, 1), lanes]
    else:
        floor, gain = stats_of(state_ref, envs, half, envs_total)
        own = state_ref[me, :, pl.ds(0, half)]
        own_ref[0:1, :] = own[0:1]
        own_ref[1:2, :] = jnp.maximum(own[1:2], floor) * gain
    per = 4

    def send(part):
        at = pl.ds(part * per * cands, per * cands)
        pair = pl.ds(part * per * 2, per * 2)
        trio = ((acts_ref, acts_out, at), (asq_ref, asq_out, at), (sums_ref, sums_out, pair))
        return [
            pltpu.make_async_copy(source.at[rows], target.at[rows], sems.at[3 * part + k])
            for k, (source, target, rows) in enumerate(trio)
        ]

    def send_own():
        return pltpu.make_async_copy(own_ref, own_out, sems.at[3 * (envs // per)])

    send_own().start()

    ids = me * cands + lax.broadcasted_iota(jnp.int32, (cands, 1), 0)
    for env in range(envs):
        at = pl.ds(env * cands, cands)
        chosen = elite_ref[it, env : env + 1, :] == ids
        member = jnp.sum(jnp.where(chosen, 1.0, 0.0), axis=1, keepdims=True)
        member = jnp.broadcast_to(member, (cands, LANES))
        square = jnp.zeros((cands, LANES), jnp.float32)
        for side in range(2):
            line = 2 * env + side
            for step in range(half // LANES):
                lanes = pl.ds(step * LANES, LANES)
                whole = pl.ds(side * half + step * LANES, LANES)
                if first:
                    center = mean_ref[pl.ds(env, 1), whole]
                    spread = std_ref[pl.ds(env, 1), whole]
                else:
                    center = state_ref[line, 0:1, lanes]
                    spread = jnp.maximum(state_ref[line, 1:2, lanes], floor) * gain
                action = jnp.clip(center + spread * noise_ref[0, at, whole], -1.0, 1.0)
                acts_ref[at, whole] = action.astype(jnp.bfloat16)
                both = action * action
                square = square + both
                sums_ref[line, 0:1, lanes] = jnp.sum(action * member, axis=0, keepdims=True)
                sums_ref[line, 1:2, lanes] = jnp.sum(both * member, axis=0, keepdims=True)
        asq_ref[at, :] = square
        if env % per == per - 1:
            for copy in send(env // per):
                copy.start()
    for part in range(envs // per):
        for copy in send(part):
            copy.wait()
    send_own().wait()


def actions_of(noise, at, elite_idx, mine, tie, state, it, envs_total, lines, half):
    _, rows, width = noise.shape
    return pl.pallas_call(
        functools.partial(action_body, it=it, envs_total=envs_total),
        grid=(1,),
        in_specs=[pl.BlockSpec((1, rows, width), lambda i: (at, 0, 0)), VMEM, SMEM, HBM]
        + [VMEM] * len(state),
        out_specs=[HBM] * 4,
        out_shape=[
            in_hbm((rows, width), jnp.bfloat16),
            in_hbm((rows, LANES)),
            in_hbm((lines, 2, half)),
            in_hbm((2, half)),
        ],
        scratch_shapes=[
            pltpu.VMEM((rows, width), jnp.bfloat16),
            pltpu.VMEM((rows, LANES), jnp.float32),
            pltpu.VMEM((lines, 2, half), jnp.float32),
            pltpu.VMEM((2, half), jnp.float32),
            pltpu.SemaphoreType.DMA((3 * (lines // 8) + 1,)),
        ],
        compiler_params=pltpu.CompilerParams(vmem_limit_bytes=12 << 20),
        name="actions",
    )(noise, elite_idx, mine, stay(tie), *state)


def refit_body(parts_ref, own_hbm, tie_ref, slice_ref, peak_ref, own_ref, sem, *, elites):
    copy = pltpu.make_async_copy(own_hbm, own_ref, sem)
    copy.start()
    total = jnp.sum(parts_ref[...], axis=0)
    copy.wait()
    mean = total[0:1] / elites
    variance = jnp.maximum(total[1:2] / elites - mean * mean, 0.0)
    slice_ref[0:1, :] = MOMENTUM * own_ref[0:1, :] + (1.0 - MOMENTUM) * mean
    mixed = MOMENTUM * own_ref[1:2, :] + (1.0 - MOMENTUM) * jnp.sqrt(variance)
    slice_ref[1:2, :] = mixed
    peak_ref[...] = jnp.broadcast_to(jnp.max(mixed, axis=1, keepdims=True)[None], peak_ref.shape)


def refit(parts, own, tie, elites, groups):
    return pl.pallas_call(
        functools.partial(refit_body, elites=elites),
        in_specs=[VMEM, HBM, HBM],
        out_specs=[VMEM, VMEM],
        out_shape=[
            jax.ShapeDtypeStruct(own.shape, jnp.float32),
            jax.ShapeDtypeStruct((groups, 1, LANES), jnp.float32),
        ],
        scratch_shapes=[pltpu.VMEM(own.shape, jnp.float32), pltpu.SemaphoreType.DMA],
        compiler_params=pltpu.CompilerParams(vmem_limit_bytes=4 << 20),
        name="refit",
    )(parts, stay(own), stay(tie))


def spread_body(slice_ref, peak_ref, out_ref, token_ref):
    lines = out_ref.shape[0]
    half = slice_ref.shape[1]
    lane = lax.broadcasted_iota(jnp.int32, (1, LANES), 1)
    tail = jnp.zeros((1, LANES), jnp.float32)
    for group in range(peak_ref.shape[0]):
        tail = jnp.where(lane == group, peak_ref[group], tail)
    main = jnp.broadcast_to(slice_ref[...][None], (lines, 2, half))
    out_ref[:, :, pl.ds(0, half)] = main
    token_ref[...] = jnp.broadcast_to(tail, token_ref.shape)
    out_ref[:, :, pl.ds(half, LANES)] = jnp.broadcast_to(tail[None], (lines, 2, LANES))


def to_all(piece, peaks, lines):
    half = piece.shape[1]
    return pl.pallas_call(
        spread_body,
        grid=(1,),
        in_specs=[VMEM, VMEM],
        out_specs=[whole((lines, 2, half + LANES)), whole((8, LANES))],
        out_shape=[in_hbm((lines, 2, half + LANES)), in_hbm((8, LANES))],
        compiler_params=pltpu.CompilerParams(vmem_limit_bytes=4 << 20),
        name="to_all",
    )(piece, peaks)


def final_body(state_ref, mean_ref, std_ref, *, envs_total):
    envs, width = mean_ref.shape
    half = width // 2
    floor, gain = stats_of(state_ref, envs, half, envs_total)
    for env in range(envs):
        for side in range(2):
            lanes = pl.ds(side * half, half)
            line = 2 * env + side
            mean_ref[pl.ds(env, 1), lanes] = state_ref[line, 0:1, pl.ds(0, half)]
            std_ref[pl.ds(env, 1), lanes] = (
                jnp.maximum(state_ref[line, 1:2, pl.ds(0, half)], floor) * gain
            )


def finished(state, envs, width, envs_total):
    shape = jax.ShapeDtypeStruct((envs, width), jnp.float32)
    return pl.pallas_call(
        functools.partial(final_body, envs_total=envs_total),
        in_specs=[VMEM],
        out_specs=[VMEM, VMEM],
        out_shape=[shape, shape],
        compiler_params=pltpu.CompilerParams(vmem_limit_bytes=4 << 20),
        name="finished",
    )(state)


def rollout_body(*refs, spans, act_dim, total, earlier):
    refs = list(refs)
    take = lambda n: [refs.pop(0) for _ in range(n)]
    acts = take(len(spans))
    carried = [take(1)[0] if first else None for first, _ in spans]
    squares = [take(1)[0] if last == total else None for _, last in spans]
    begin_ref, goal_ref, ws_ref, wa_ref, wout_ref, bin_ref, bout_ref = take(7)
    before = take(earlier)
    take(1)
    outs = take(len(spans))
    moves, win, start, goal, sems = refs
    envs, dim = begin_ref.shape
    rows = acts[0].shape[0]
    cands = rows // envs
    steps = spans[0][1] - spans[0][0]
    copies = []
    for k, (first, last) in enumerate(spans):
        copies.append(
            pltpu.make_async_copy(
                acts[k].at[:, pl.ds(first * act_dim, steps * act_dim)],
                moves.at[pl.ds(k * rows, rows), :],
                sems.at[k],
            )
        )
        copies[k].start()
    zeros = jnp.zeros(wa_ref.shape, jnp.bfloat16)
    for parity in range(2):
        win[parity, pl.ds(0, dim), :] = ws_ref[...] * jnp.bfloat16(0.5)
        win[parity, pl.ds(dim + parity * act_dim, act_dim), :] = wa_ref[...] * jnp.bfloat16(0.5)
        win[parity, pl.ds(dim + (1 - parity) * act_dim, act_dim), :] = zeros
    for k in range(len(spans)):
        for env in range(envs):
            at = pl.ds(k * rows + env * cands, cands)
            if carried[k] is None:
                start[0, at, :] = jnp.broadcast_to(begin_ref[pl.ds(env, 1), :], (cands, dim))
            goal[at, :] = jnp.broadcast_to(goal_ref[pl.ds(env, 1), :], (cands, dim))
        at = pl.ds(k * rows, rows)
        if carried[k] is None:
            start[1, at, :] = jnp.zeros((rows, dim), jnp.float32)
        else:
            start[0, at, :] = carried[k][0]
            start[1, at, :] = carried[k][1]
    bias_in = bin_ref[...] * 0.5
    for copy in copies:
        copy.wait()

    def two_steps(k, carry):
        state, error = carry
        pair = moves[:, pl.ds(pl.multiple_of(k * 2 * act_dim, 2 * act_dim), 2 * act_dim)]
        for parity in range(2):
            joined = jnp.concatenate([state.astype(jnp.bfloat16), pair], axis=1)
            half = jnp.dot(joined, win[parity], preferred_element_type=jnp.float32) + bias_in
            hidden = (half + half * jnp.tanh(half)).astype(jnp.bfloat16)
            moved = jnp.dot(hidden, wout_ref[...], preferred_element_type=jnp.float32)
            state = jnp.tanh(state + moved + bout_ref[...])
            gap = state - goal[...]
            error = error + gap * gap
        return state, error

    state, error = lax.fori_loop(0, steps // 2, two_steps, (start[0], start[1]))
    for k, (_, last) in enumerate(spans):
        part = slice(k * rows, (k + 1) * rows)
        if last < total:
            outs[k][0] = state[part]
            outs[k][1] = error[part]
            continue
        both = error[part] / (dim * total) + squares[k][...] * (ACT_COST / (act_dim * total))
        cost = jnp.broadcast_to(jnp.sum(both, axis=1, keepdims=True), (rows, LANES))
        lane = lax.broadcasted_iota(jnp.int32, (cands, LANES), 1)
        table = jnp.zeros((cands, LANES), jnp.float32)
        for env in range(envs):
            table = jnp.where(lane == env, cost[env * cands : (env + 1) * cands], table)
        for n in range(earlier):
            outs[k][n] = before[n][0]
        outs[k][earlier] = table[:, :envs]


def rollout(parts, fixed, before, tie, act_dim):
    rows, width = parts[0][0].shape
    envs, dim = fixed[0].shape
    cands = rows // envs
    total = width // act_dim
    spans = [(p[3], p[4]) for p in parts]
    steps = spans[0][1] - spans[0][0]
    assert all(b - a == steps and a % 2 == 0 for a, b in spans) and steps % 2 == 0
    acts = [p[0] for p in parts]
    carried = [p[2] for p in parts if p[3]]
    squares = [p[1] for p in parts if p[4] == total]
    shapes = [
        (1 + len(before), cands, envs) if last == total else (2, rows, dim) for _, last in spans
    ]
    small = len(carried) + len(squares) + len(fixed) + len(before)
    return pl.pallas_call(
        functools.partial(
            rollout_body, spans=spans, act_dim=act_dim, total=total, earlier=len(before)
        ),
        grid=(1,),
        in_specs=[HBM] * len(acts) + [VMEM] * small + [HBM],
        out_specs=[whole(shape) for shape in shapes],
        out_shape=[in_hbm(shape) for shape in shapes],
        scratch_shapes=[
            pltpu.VMEM((len(parts) * rows, steps * act_dim), jnp.bfloat16),
            pltpu.VMEM((2, dim + 2 * act_dim, fixed[2].shape[1]), jnp.bfloat16),
            pltpu.VMEM((2, len(parts) * rows, dim), jnp.float32),
            pltpu.VMEM((len(parts) * rows, dim), jnp.float32),
            pltpu.SemaphoreType.DMA((len(parts),)),
        ],
        cost_estimate=pl.CostEstimate(flops=ROLL_FLOPS, bytes_accessed=1 << 20, transcendentals=0),
        compiler_params=pltpu.CompilerParams(vmem_limit_bytes=10 << 20),
        name="rollout",
    )(*map(stay, acts), *carried, *squares, *fixed, *before, stay(tie))


def shards(
    white,
    mean_init,
    std_init,
    init_state,
    goal_state,
    w_state,
    w_action,
    w_out,
    bias_in,
    bias_out,
    elite_idx,
):
    iters, envs, cands, flat = white.shape
    act_dim = w_action.shape[0]
    length = flat // act_dim
    width = mean_init.shape[1]
    horizon = width // act_dim
    half = width // 2
    elites = elite_idx.shape[2]
    groups = lax.axis_size("env")
    peers = lax.axis_size("cand")
    lines = 2 * envs
    envs_total = envs * groups
    rows = envs * cands
    assert lines == peers and rows % 16 == 0
    assert iters == 3 and horizon == 40
    mine = lax.axis_index("cand").astype(jnp.int32)[None]
    fixed = (init_state, goal_state, w_state, w_action, w_out, bias_in[None], bias_out[None])
    white = white.reshape(iters, rows, flat)
    elite_idx = jnp.swapaxes(elite_idx, 0, 1)
    mix = functools.partial(lax.all_to_all, axis_name="cand", split_axis=0, concat_axis=0, tiled=True)
    acts, asq, held, costs = {}, {}, {}, {}

    def part(it, first, last):
        return (acts[it], asq[it], held.get(it), first, last)

    def play(parts, tie, before=()):
        outs = rollout([part(*p) for p in parts], fixed, before, tie, act_dim)
        for (it, _, last), out in zip(parts, outs):
            if last < horizon:
                held[it] = out
            else:
                costs[it] = out
        return outs[0]

    noise, _ = noise_of(white, 0, 1, mine, act_dim, horizon)
    state, tie = (mean_init, std_init), mine
    for it in range(iters):
        acts[it], asq[it], sums, own = actions_of(
            noise, max(it - 1, 0), elite_idx, mine, tie, state, it, envs_total, lines, half
        )
        parts = mix(sums)
        if it == 0:
            noise, tie = noise_of(white, 1, iters - 1, own, act_dim, horizon)
        elif it == 1:
            tie = play([(0, 14, 26), (1, 0, 12)], own)
        else:
            tie = play([(1, 26, horizon), (2, 0, 14)], own)
        piece, peak = refit(parts, own, tie, elites, groups)
        peaks = lax.all_to_all(peak, "env", 0, 0, tiled=True)
        spread, token = to_all(piece, peaks, lines)
        state = (mix(spread),)
        if it == 0:
            tie = play([(0, 0, 14)], token)
        elif it == 1:
            tie = play([(0, 26, horizon), (1, 12, 26)], token)
        else:
            tie = play([(2, 14, horizon)], token, (costs[0], costs[1]))
    mean, std = finished(state[0], envs, width, envs_total)
    return (mean, std, jnp.swapaxes(costs[iters - 1], 1, 2))


def solution(mesh):
    in_specs = (
        P(None, "env", "cand", None),
        P("env", None),
        P("env", None),
        P("env", None),
        P("env", None),
        P(),
        P(),
        P(),
        P(),
        P(),
        P("env", None, None),
    )
    out_specs = (P("env", None), P("env", None), P(None, "env", "cand"))
    return jax.shard_map(shards, mesh=mesh, in_specs=in_specs, out_specs=out_specs, check_vma=False)
```

```python
import functools

import jax
import jax.numpy as jnp
import numpy as np
from jax import lax
from jax.experimental import pallas as pl
from jax.experimental.pallas import tpu as pltpu
from jax.sharding import PartitionSpec as P

BETA_EXP = 2.5
MOMENTUM = 0.1
FLOOR_SHARE = 0.1
ACT_COST = 0.1
LANES = 128
ROLL_FLOPS = 1 << 28
VMEM = pl.BlockSpec(memory_space=pltpu.VMEM)
SMEM = pl.BlockSpec(memory_space=pltpu.SMEM)
HBM = pl.BlockSpec(memory_space=pltpu.HBM)


def whole(shape):
    return pl.BlockSpec(shape, lambda i: (0,) * len(shape))


def stay(array):
    return pltpu.with_memory_space_constraint(array, pltpu.HBM)


def in_hbm(shape, dtype=jnp.float32):
    return pltpu.HBM(shape, dtype)


def color_kernel(length):
    freqs = np.arange(length // 2 + 1)
    scale = (np.maximum(freqs, 1).astype(np.float32) / np.float32(length)) ** np.float32(-BETA_EXP / 2)
    kernel = np.fft.irfft(scale.astype(np.float64), n=length)
    kernel = kernel / np.sqrt(np.sum(kernel * kernel))
    return np.asarray(kernel, np.float32).astype(jnp.bfloat16).astype(np.float32)


def noise_body(white_ref, own_ref, out_ref, same_ref, rows_in, fill, sems, *, act_dim, blocks, first, parts):
    count = out_ref.shape[0]
    _, rows, flat = white_ref.shape
    length = flat // act_dim
    size = rows // parts

    def fetch(one, part):
        at = pl.ds(part * size, size)
        return pltpu.make_async_copy(
            white_ref.at[first + one, at, :], rows_in.at[one, at, :], sems.at[one * parts + part]
        )

    for one in range(count):
        for part in range(parts):
            fetch(one, part).start()
    kernel = color_kernel(length)
    row = lax.broadcasted_iota(jnp.int32, (act_dim, 256), 0)
    lane = lax.broadcasted_iota(jnp.int32, (act_dim, 256), 1)
    hit = lane % act_dim == row
    quarter = lax.broadcasted_iota(jnp.int32, (1, 256), 1) // act_dim
    for j in range(length):
        band = jnp.full((1, 256), float(kernel[-j % length]), jnp.float32)
        for q in range(1, 256 // act_dim):
            band = jnp.where(quarter == q, float(kernel[(q - j) % length]), band)
        tile = jnp.where(hit, band, 0.0).astype(jnp.bfloat16)
        fill[pl.ds(j * act_dim, act_dim), :] = tile
        fill[pl.ds(flat + j * act_dim, act_dim), :] = tile
    for one in range(count):
        for part in range(parts):
            fetch(one, part).wait()
        for block in range(blocks):
            start = (flat - block * 256) % flat
            out_ref[one, :, pl.ds(block * 256, 256)] = jnp.dot(
                rows_in[one], fill[pl.ds(start, flat), :], preferred_element_type=jnp.float32
            )
    same_ref[...] = own_ref[...]


def noise_of(white, first, count, own, act_dim, horizon):
    _, rows, flat = white.shape
    width = horizon * act_dim
    parts = 1
    return pl.pallas_call(
        functools.partial(
            noise_body, act_dim=act_dim, blocks=width // 256, first=first, parts=parts
        ),
        grid=(1,),
        in_specs=[HBM, whole(own.shape)],
        out_specs=[VMEM, VMEM],
        out_shape=[
            jax.ShapeDtypeStruct((count, rows, width), jnp.float32),
            jax.ShapeDtypeStruct(own.shape, own.dtype),
        ],
        scratch_shapes=[
            pltpu.VMEM((count, rows, flat), jnp.bfloat16),
            pltpu.VMEM((2 * flat, 256), jnp.bfloat16),
            pltpu.SemaphoreType.DMA((count * parts,)),
        ],
        cost_estimate=pl.CostEstimate(flops=ROLL_FLOPS, bytes_accessed=1 << 20, transcendentals=0),
        compiler_params=pltpu.CompilerParams(vmem_limit_bytes=16 << 20),
        name="noise",
    )(stay(white), stay(own))


def stats_of(state_ref, envs, half, envs_total):
    peaks = state_ref[:, 0, pl.ds(half, LANES)]
    pair = jnp.max(peaks.reshape(envs, 2, LANES), axis=1)
    peak = jnp.max(pair, axis=(0, 1), keepdims=True)
    total = jnp.sum(jnp.sum(pair, axis=0, keepdims=True), axis=1, keepdims=True)
    return FLOOR_SHARE * peak, 0.5 + total / (peak * envs_total)


def action_body(*refs, it, envs_total):
    first = it == 0
    if first:
        noise_ref, elite_ref, mine_ref, tie_ref, mean_ref, std_ref = refs[:6]
    else:
        noise_ref, elite_ref, mine_ref, tie_ref, state_ref = refs[:5]
    acts_out, asq_out, sums_out, own_out, acts_ref, asq_ref, sums_ref, own_ref, sems = refs[-9:]
    half = sums_ref.shape[2]
    rows = acts_ref.shape[0]
    envs = sums_ref.shape[0] // 2
    cands = rows // envs
    me = mine_ref[0]
    if first:
        lanes = pl.ds(pl.multiple_of((me % 2) * half, LANES), half)
        own_ref[0:1, :] = mean_ref[pl.ds(me // 2, 1), lanes]
        own_ref[1:2, :] = std_ref[pl.ds(me // 2, 1), lanes]
    else:
        floor, gain = stats_of(state_ref, envs, half, envs_total)
        own = state_ref[me, :, pl.ds(0, half)]
        own_ref[0:1, :] = own[0:1]
        own_ref[1:2, :] = jnp.maximum(own[1:2], floor) * gain
    per = 4

    def send(part):
        at = pl.ds(part * per * cands, per * cands)
        pair = pl.ds(part * per * 2, per * 2)
        trio = ((acts_ref, acts_out, at), (asq_ref, asq_out, at), (sums_ref, sums_out, pair))
        return [
            pltpu.make_async_copy(source.at[rows], target.at[rows], sems.at[3 * part + k])
            for k, (source, target, rows) in enumerate(trio)
        ]

    def send_own():
        return pltpu.make_async_copy(own_ref, own_out, sems.at[3 * (envs // per)])

    send_own().start()

    ids = me * cands + lax.broadcasted_iota(jnp.int32, (cands, 1), 0)
    for env in range(envs):
        at = pl.ds(env * cands, cands)
        chosen = elite_ref[it, env : env + 1, :] == ids
        member = jnp.sum(jnp.where(chosen, 1.0, 0.0), axis=1, keepdims=True)
        member = jnp.broadcast_to(member, (cands, LANES))
        square = jnp.zeros((cands, LANES), jnp.float32)
        for side in range(2):
            line = 2 * env + side
            for step in range(half // LANES):
                lanes = pl.ds(step * LANES, LANES)
                whole = pl.ds(side * half + step * LANES, LANES)
                if first:
                    center = mean_ref[pl.ds(env, 1), whole]
                    spread = std_ref[pl.ds(env, 1), whole]
                else:
                    center = state_ref[line, 0:1, lanes]
                    spread = jnp.maximum(state_ref[line, 1:2, lanes], floor) * gain
                action = jnp.clip(center + spread * noise_ref[0, at, whole], -1.0, 1.0)
                acts_ref[at, whole] = action.astype(jnp.bfloat16)
                both = action * action
                square = square + both
                sums_ref[line, 0:1, lanes] = jnp.sum(action * member, axis=0, keepdims=True)
                sums_ref[line, 1:2, lanes] = jnp.sum(both * member, axis=0, keepdims=True)
        asq_ref[at, :] = square
        if env % per == per - 1:
            for copy in send(env // per):
                copy.start()
    for part in range(envs // per):
        for copy in send(part):
            copy.wait()
    send_own().wait()


def actions_of(noise, at, elite_idx, mine, tie, state, it, envs_total, lines, half):
    _, rows, width = noise.shape
    return pl.pallas_call(
        functools.partial(action_body, it=it, envs_total=envs_total),
        grid=(1,),
        in_specs=[pl.BlockSpec((1, rows, width), lambda i: (at, 0, 0)), VMEM, SMEM, HBM]
        + [VMEM] * len(state),
        out_specs=[HBM] * 4,
        out_shape=[
            in_hbm((rows, width), jnp.bfloat16),
            in_hbm((rows, LANES)),
            in_hbm((lines, 2, half)),
            in_hbm((2, half)),
        ],
        scratch_shapes=[
            pltpu.VMEM((rows, width), jnp.bfloat16),
            pltpu.VMEM((rows, LANES), jnp.float32),
            pltpu.VMEM((lines, 2, half), jnp.float32),
            pltpu.VMEM((2, half), jnp.float32),
            pltpu.SemaphoreType.DMA((3 * (lines // 8) + 1,)),
        ],
        compiler_params=pltpu.CompilerParams(vmem_limit_bytes=12 << 20),
        name="actions",
    )(noise, elite_idx, mine, stay(tie), *state)


def refit_body(parts_ref, own_ref, slice_ref, peak_ref, *, elites):
    total = jnp.sum(parts_ref[...], axis=0)
    mean = total[0:1] / elites
    variance = jnp.maximum(total[1:2] / elites - mean * mean, 0.0)
    slice_ref[0:1, :] = MOMENTUM * own_ref[0:1, :] + (1.0 - MOMENTUM) * mean
    mixed = MOMENTUM * own_ref[1:2, :] + (1.0 - MOMENTUM) * jnp.sqrt(variance)
    slice_ref[1:2, :] = mixed
    peak_ref[...] = jnp.broadcast_to(jnp.max(mixed, axis=1, keepdims=True)[None], peak_ref.shape)


def refit(parts, own, elites, groups):
    return pl.pallas_call(
        functools.partial(refit_body, elites=elites),
        in_specs=[VMEM, VMEM],
        out_specs=[VMEM, VMEM],
        out_shape=[
            jax.ShapeDtypeStruct(own.shape, jnp.float32),
            jax.ShapeDtypeStruct((groups, 1, LANES), jnp.float32),
        ],
        compiler_params=pltpu.CompilerParams(vmem_limit_bytes=4 << 20),
        name="refit",
    )(parts, own)


def spread_body(slice_ref, peak_ref, tie_ref, out_ref, token_ref):
    lines = out_ref.shape[0]
    half = slice_ref.shape[1]
    lane = lax.broadcasted_iota(jnp.int32, (1, LANES), 1)
    tail = jnp.zeros((1, LANES), jnp.float32)
    for group in range(peak_ref.shape[0]):
        tail = jnp.where(lane == group, peak_ref[group], tail)
    main = jnp.broadcast_to(slice_ref[...][None], (lines, 2, half))
    out_ref[:, :, pl.ds(0, half)] = main
    token_ref[...] = jnp.broadcast_to(tail, token_ref.shape)
    out_ref[:, :, pl.ds(half, LANES)] = jnp.broadcast_to(tail[None], (lines, 2, LANES))


def to_all(piece, peaks, tie, lines):
    half = piece.shape[1]
    return pl.pallas_call(
        spread_body,
        grid=(1,),
        in_specs=[VMEM, VMEM, HBM],
        out_specs=[whole((lines, 2, half + LANES)), whole((8, LANES))],
        out_shape=[in_hbm((lines, 2, half + LANES)), in_hbm((8, LANES))],
        compiler_params=pltpu.CompilerParams(vmem_limit_bytes=4 << 20),
        name="to_all",
    )(piece, peaks, stay(tie))


def final_body(state_ref, mean_ref, std_ref, *, envs_total):
    envs, width = mean_ref.shape
    half = width // 2
    floor, gain = stats_of(state_ref, envs, half, envs_total)
    for env in range(envs):
        for side in range(2):
            lanes = pl.ds(side * half, half)
            line = 2 * env + side
            mean_ref[pl.ds(env, 1), lanes] = state_ref[line, 0:1, pl.ds(0, half)]
            std_ref[pl.ds(env, 1), lanes] = (
                jnp.maximum(state_ref[line, 1:2, pl.ds(0, half)], floor) * gain
            )


def finished(state, envs, width, envs_total):
    shape = jax.ShapeDtypeStruct((envs, width), jnp.float32)
    return pl.pallas_call(
        functools.partial(final_body, envs_total=envs_total),
        in_specs=[VMEM],
        out_specs=[VMEM, VMEM],
        out_shape=[shape, shape],
        compiler_params=pltpu.CompilerParams(vmem_limit_bytes=4 << 20),
        name="finished",
    )(state)


def rollout_body(*refs, spans, act_dim, total, earlier, keep):
    refs = list(refs)
    take = lambda n: [refs.pop(0) for _ in range(n)]
    acts = take(len(spans))
    carried = [take(1)[0] if first else None for first, _ in spans]
    squares = [take(1)[0] if last == total else None for _, last in spans]
    begin_ref, goal_ref, ws_ref, wa_ref, wout_ref, bin_ref, bout_ref = take(7)
    before = take(earlier)
    tie_ref = take(1)[0]
    outs = take(len(spans))
    if keep:
        take(1)[0][...] = tie_ref[...]
    moves, win, start, goal, sems = refs
    envs, dim = begin_ref.shape
    rows = acts[0].shape[0]
    cands = rows // envs
    steps = spans[0][1] - spans[0][0]
    copies = []
    for k, (first, last) in enumerate(spans):
        copies.append(
            pltpu.make_async_copy(
                acts[k].at[:, pl.ds(first * act_dim, steps * act_dim)],
                moves.at[pl.ds(k * rows, rows), :],
                sems.at[k],
            )
        )
        copies[k].start()
    zeros = jnp.zeros(wa_ref.shape, jnp.bfloat16)
    for parity in range(2):
        win[parity, pl.ds(0, dim), :] = ws_ref[...] * jnp.bfloat16(0.5)
        win[parity, pl.ds(dim + parity * act_dim, act_dim), :] = wa_ref[...] * jnp.bfloat16(0.5)
        win[parity, pl.ds(dim + (1 - parity) * act_dim, act_dim), :] = zeros
    for k in range(len(spans)):
        for env in range(envs):
            at = pl.ds(k * rows + env * cands, cands)
            if carried[k] is None:
                start[0, at, :] = jnp.broadcast_to(begin_ref[pl.ds(env, 1), :], (cands, dim))
            goal[at, :] = jnp.broadcast_to(goal_ref[pl.ds(env, 1), :], (cands, dim))
        at = pl.ds(k * rows, rows)
        if carried[k] is None:
            start[1, at, :] = jnp.zeros((rows, dim), jnp.float32)
        else:
            start[0, at, :] = carried[k][0]
            start[1, at, :] = carried[k][1]
    bias_in = bin_ref[...] * 0.5
    for copy in copies:
        copy.wait()

    many = 4 if steps % 4 == 0 else 2

    def some_steps(k, carry):
        state, error = carry
        for n in range(many):
            parity = n % 2
            at = pl.multiple_of((k * many + n - parity) * act_dim, 2 * act_dim)
            pair = moves[:, pl.ds(at, 2 * act_dim)]
            joined = jnp.concatenate([state.astype(jnp.bfloat16), pair], axis=1)
            half = jnp.dot(joined, win[parity], preferred_element_type=jnp.float32) + bias_in
            hidden = (half + half * jnp.tanh(half)).astype(jnp.bfloat16)
            moved = jnp.dot(hidden, wout_ref[...], preferred_element_type=jnp.float32)
            state = jnp.tanh(state + moved + bout_ref[...])
            gap = state - goal[...]
            error = error + gap * gap
        return state, error

    state, error = lax.fori_loop(0, steps // many, some_steps, (start[0], start[1]))
    for k, (_, last) in enumerate(spans):
        part = slice(k * rows, (k + 1) * rows)
        if last < total:
            outs[k][0] = state[part]
            outs[k][1] = error[part]
            continue
        both = error[part] / (dim * total) + squares[k][...] * (ACT_COST / (act_dim * total))
        cost = jnp.broadcast_to(jnp.sum(both, axis=1, keepdims=True), (rows, LANES))
        lane = lax.broadcasted_iota(jnp.int32, (cands, LANES), 1)
        table = jnp.zeros((cands, LANES), jnp.float32)
        for env in range(envs):
            table = jnp.where(lane == env, cost[env * cands : (env + 1) * cands], table)
        for n in range(earlier):
            outs[k][n] = before[n][0]
        outs[k][earlier] = table[:, :envs]


def rollout(parts, fixed, before, tie, act_dim, keep):
    rows, width = parts[0][0].shape
    envs, dim = fixed[0].shape
    cands = rows // envs
    total = width // act_dim
    spans = [(p[3], p[4]) for p in parts]
    steps = spans[0][1] - spans[0][0]
    assert all(b - a == steps and a % 2 == 0 for a, b in spans) and steps % 2 == 0
    acts = [p[0] for p in parts]
    carried = [p[2] for p in parts if p[3]]
    squares = [p[1] for p in parts if p[4] == total]
    shapes = [
        (1 + len(before), cands, envs) if last == total else (2, rows, dim) for _, last in spans
    ]
    loose = carried + squares
    return pl.pallas_call(
        functools.partial(
            rollout_body, spans=spans, act_dim=act_dim, total=total, earlier=len(before), keep=keep
        ),
        grid=(1,),
        in_specs=[HBM] * len(acts)
        + [whole(a.shape) for a in loose]
        + [VMEM] * len(fixed)
        + [whole(a.shape) for a in before]
        + [whole(tie.shape) if keep else HBM],
        out_specs=[whole(shape) for shape in shapes] + [VMEM] * keep,
        out_shape=[in_hbm(shape) for shape in shapes]
        + [jax.ShapeDtypeStruct(tie.shape, tie.dtype)] * keep,
        scratch_shapes=[
            pltpu.VMEM((len(parts) * rows, steps * act_dim), jnp.bfloat16),
            pltpu.VMEM((2, dim + 2 * act_dim, fixed[2].shape[1]), jnp.bfloat16),
            pltpu.VMEM((2, len(parts) * rows, dim), jnp.float32),
            pltpu.VMEM((len(parts) * rows, dim), jnp.float32),
            pltpu.SemaphoreType.DMA((len(parts),)),
        ],
        cost_estimate=pl.CostEstimate(flops=ROLL_FLOPS, bytes_accessed=1 << 20, transcendentals=0),
        compiler_params=pltpu.CompilerParams(vmem_limit_bytes=10 << 20),
        name="rollout",
    )(*map(stay, acts), *map(stay, loose), *fixed, *map(stay, before), stay(tie))


def shards(
    white,
    mean_init,
    std_init,
    init_state,
    goal_state,
    w_state,
    w_action,
    w_out,
    bias_in,
    bias_out,
    elite_idx,
):
    iters, envs, cands, flat = white.shape
    act_dim = w_action.shape[0]
    length = flat // act_dim
    width = mean_init.shape[1]
    horizon = width // act_dim
    half = width // 2
    elites = elite_idx.shape[2]
    groups = lax.axis_size("env")
    peers = lax.axis_size("cand")
    lines = 2 * envs
    envs_total = envs * groups
    rows = envs * cands
    assert lines == peers and rows % 16 == 0
    assert iters == 3 and horizon == 40
    mine = lax.axis_index("cand").astype(jnp.int32)[None]
    fixed = (init_state, goal_state, w_state, w_action, w_out, bias_in[None], bias_out[None])
    white = white.reshape(iters, rows, flat)
    elite_idx = jnp.swapaxes(elite_idx, 0, 1)
    mix = functools.partial(lax.all_to_all, axis_name="cand", split_axis=0, concat_axis=0, tiled=True)
    acts, asq, held, costs = {}, {}, {}, {}

    def part(it, first, last):
        return (acts[it], asq[it], held.get(it), first, last)

    def play(parts, tie, before=(), keep=False):
        outs = rollout([part(*p) for p in parts], fixed, before, tie, act_dim, keep)
        for (it, _, last), out in zip(parts, outs):
            if last < horizon:
                held[it] = out
            else:
                costs[it] = out
        return outs[-1] if keep else outs[0]

    noise, _ = noise_of(white, 0, 1, bias_out[None], act_dim, horizon)
    state, tie = (mean_init, std_init), mine
    for it in range(iters):
        acts[it], asq[it], sums, own = actions_of(
            noise, max(it - 1, 0), elite_idx, mine, tie, state, it, envs_total, lines, half
        )
        parts = mix(sums)
        if it == 0:
            noise, own = noise_of(white, 1, iters - 1, own, act_dim, horizon)
        elif it == 1:
            own = play([(0, 14, 26), (1, 0, 12)], own, keep=True)
        else:
            own = play([(1, 26, horizon), (2, 0, 14)], own, keep=True)
        piece, peak = refit(parts, own, elites, groups)
        peaks = lax.all_to_all(peak, "env", 0, 0, tiled=True)
        tie = mine if it < iters - 1 else play([(2, 14, 20)], peak)
        spread, token = to_all(piece, peaks, tie, lines)
        state = (mix(spread),)
        if it == 0:
            tie = play([(0, 0, 14)], token)
        elif it == 1:
            tie = play([(0, 26, horizon), (1, 12, 26)], token)
        else:
            tie = play([(2, 20, horizon)], token, (costs[0], costs[1]))
    mean, std = finished(state[0], envs, width, envs_total)
    return (mean, std, jnp.swapaxes(costs[iters - 1], 1, 2))


def solution(mesh):
    in_specs = (
        P(None, "env", "cand", None),
        P("env", None),
        P("env", None),
        P("env", None),
        P("env", None),
        P(),
        P(),
        P(),
        P(),
        P(),
        P("env", None, None),
    )
    out_specs = (P("env", None), P("env", None), P(None, "env", "cand"))
    return jax.shard_map(shards, mesh=mesh, in_specs=in_specs, out_specs=out_specs, check_vma=False)
```

```python
import functools

import jax
import jax.numpy as jnp
import numpy as np
from jax import lax
from jax.experimental import pallas as pl
from jax.experimental.pallas import tpu as pltpu
from jax.sharding import PartitionSpec as P

BETA_EXP = 2.5
MOMENTUM = 0.1
FLOOR_SHARE = 0.1
ACT_COST = 0.1
LANES = 128
SLOTS = 8
ROLL_FLOPS = 1 << 28
VMEM = pl.BlockSpec(memory_space=pltpu.VMEM)
SMEM = pl.BlockSpec(memory_space=pltpu.SMEM)
HBM = pl.BlockSpec(memory_space=pltpu.HBM)


def whole(shape):
    return pl.BlockSpec(shape, lambda i: (0,) * len(shape))


def stay(array):
    return pltpu.with_memory_space_constraint(array, pltpu.HBM)


def in_hbm(shape, dtype=jnp.float32):
    return pltpu.HBM(shape, dtype)


def color_kernel(length):
    freqs = np.arange(length // 2 + 1)
    scale = (np.maximum(freqs, 1).astype(np.float32) / np.float32(length)) ** np.float32(-BETA_EXP / 2)
    kernel = np.fft.irfft(scale.astype(np.float64), n=length)
    kernel = kernel / np.sqrt(np.sum(kernel * kernel))
    return np.asarray(kernel, np.float32).astype(jnp.bfloat16).astype(np.float32)


def noise_body(*refs, act_dim, blocks, first, parts, keep):
    white_ref, out_ref, rows_in, fill, sems = refs[0], refs[1 + keep], *refs[-3:]
    count = out_ref.shape[0]
    if keep:
        hand = pltpu.make_async_copy(refs[1], refs[3], sems.at[count * parts])
        hand.start()
    _, rows, flat = white_ref.shape
    length = flat // act_dim
    size = rows // parts

    def fetch(one, part):
        at = pl.ds(part * size, size)
        return pltpu.make_async_copy(
            white_ref.at[first + one, at, :], rows_in.at[one, at, :], sems.at[one * parts + part]
        )

    for one in range(count):
        for part in range(parts):
            fetch(one, part).start()
    kernel = color_kernel(length)
    row = lax.broadcasted_iota(jnp.int32, (act_dim, 256), 0)
    lane = lax.broadcasted_iota(jnp.int32, (act_dim, 256), 1)
    hit = lane % act_dim == row
    quarter = lax.broadcasted_iota(jnp.int32, (1, 256), 1) // act_dim
    for j in range(length):
        band = jnp.full((1, 256), float(kernel[-j % length]), jnp.float32)
        for q in range(1, 256 // act_dim):
            band = jnp.where(quarter == q, float(kernel[(q - j) % length]), band)
        tile = jnp.where(hit, band, 0.0).astype(jnp.bfloat16)
        fill[pl.ds(j * act_dim, act_dim), :] = tile
        fill[pl.ds(flat + j * act_dim, act_dim), :] = tile
    for one in range(count):
        for part in range(parts):
            fetch(one, part).wait()
        for block in range(blocks):
            start = (flat - block * 256) % flat
            out_ref[one, :, pl.ds(block * 256, 256)] = jnp.dot(
                rows_in[one], fill[pl.ds(start, flat), :], preferred_element_type=jnp.float32
            )
    if keep:
        hand.wait()


def noise_of(white, first, count, own, act_dim, horizon):
    _, rows, flat = white.shape
    width = horizon * act_dim
    parts = 1
    keep = own is not None
    shapes = [jax.ShapeDtypeStruct((count, rows, width), jnp.float32)]
    if keep:
        shapes.append(jax.ShapeDtypeStruct(own.shape, own.dtype))
    return pl.pallas_call(
        functools.partial(
            noise_body, act_dim=act_dim, blocks=width // 256, first=first, parts=parts, keep=keep
        ),
        in_specs=[HBM] * (1 + keep),
        out_specs=[VMEM] * (1 + keep),
        out_shape=shapes,
        scratch_shapes=[
            pltpu.VMEM((count, rows, flat), jnp.bfloat16),
            pltpu.VMEM((2 * flat, 256), jnp.bfloat16),
            pltpu.SemaphoreType.DMA((count * parts + 1,)),
        ],
        cost_estimate=pl.CostEstimate(flops=ROLL_FLOPS, bytes_accessed=1 << 20, transcendentals=0),
        compiler_params=pltpu.CompilerParams(vmem_limit_bytes=16 << 20),
        name="noise",
    )(stay(white), *([stay(own)] if keep else []))


def stats_of(state_ref, envs, half, envs_total):
    peaks = state_ref[:, 0, pl.ds(half, LANES)]
    pair = jnp.max(peaks.reshape(envs, 2, LANES), axis=1)
    peak = jnp.max(pair, axis=(0, 1), keepdims=True)
    total = jnp.sum(jnp.sum(pair, axis=0, keepdims=True), axis=1, keepdims=True)
    return FLOOR_SHARE * peak, 0.5 + total / (peak * envs_total)


def action_body(*refs, it, envs_total):
    first = it == 0
    if first:
        noise_ref, elite_ref, mine_ref, tie_ref, mean_ref, std_ref = refs[:6]
    else:
        noise_ref, elite_ref, mine_ref, tie_ref, state_ref = refs[:5]
    acts_out, asq_out, sums_out, own_out, acts_ref, asq_ref, sums_ref, own_ref, sems = refs[-9:]
    half = sums_ref.shape[2]
    rows = acts_ref.shape[0]
    envs = sums_ref.shape[0] // 2
    cands = rows // envs
    me = mine_ref[0]
    if first:
        lanes = pl.ds(pl.multiple_of((me % 2) * half, LANES), half)
        own_ref[0:1, :] = mean_ref[pl.ds(me // 2, 1), lanes]
        own_ref[1:2, :] = std_ref[pl.ds(me // 2, 1), lanes]
    else:
        floor, gain = stats_of(state_ref, envs, half, envs_total)
        own = state_ref[me, :, pl.ds(0, half)]
        own_ref[0:1, :] = own[0:1]
        own_ref[1:2, :] = jnp.maximum(own[1:2], floor) * gain
    per = 4

    def send(part):
        at = pl.ds(part * per * cands, per * cands)
        pair = pl.ds(part * per * 2, per * 2)
        trio = ((acts_ref, acts_out, at), (asq_ref, asq_out, at), (sums_ref, sums_out, pair))
        return [
            pltpu.make_async_copy(source.at[rows], target.at[rows], sems.at[3 * part + k])
            for k, (source, target, rows) in enumerate(trio)
        ]

    def send_own():
        return pltpu.make_async_copy(own_ref, own_out, sems.at[3 * (envs // per)])

    send_own().start()

    ids = me * cands + lax.broadcasted_iota(jnp.int32, (cands, 1), 0)
    for env in range(envs):
        at = pl.ds(env * cands, cands)
        chosen = elite_ref[it, env : env + 1, :] == ids
        member = jnp.sum(jnp.where(chosen, 1.0, 0.0), axis=1, keepdims=True)
        member = jnp.broadcast_to(member, (cands, LANES))
        square = jnp.zeros((cands, LANES), jnp.float32)
        for side in range(2):
            line = 2 * env + side
            for step in range(half // LANES):
                lanes = pl.ds(step * LANES, LANES)
                whole = pl.ds(side * half + step * LANES, LANES)
                if first:
                    center = mean_ref[pl.ds(env, 1), whole]
                    spread = std_ref[pl.ds(env, 1), whole]
                else:
                    center = state_ref[line, 0:1, lanes]
                    spread = jnp.maximum(state_ref[line, 1:2, lanes], floor) * gain
                action = jnp.clip(center + spread * noise_ref[0, at, whole], -1.0, 1.0)
                acts_ref[at, whole] = action.astype(jnp.bfloat16)
                both = action * action
                square = square + both
                sums_ref[line, 0:1, lanes] = jnp.sum(action * member, axis=0, keepdims=True)
                sums_ref[line, 1:2, lanes] = jnp.sum(both * member, axis=0, keepdims=True)
        asq_ref[at, :] = square
        if env % per == per - 1:
            for copy in send(env // per):
                copy.start()
    for part in range(envs // per):
        for copy in send(part):
            copy.wait()
    send_own().wait()


def actions_of(noise, at, elite_idx, mine, tie, state, it, envs_total, lines, half):
    _, rows, width = noise.shape
    return pl.pallas_call(
        functools.partial(action_body, it=it, envs_total=envs_total),
        grid=(1,),
        in_specs=[pl.BlockSpec((1, rows, width), lambda i: (at, 0, 0)), VMEM, SMEM, HBM]
        + [VMEM] * len(state),
        out_specs=[HBM] * 4,
        out_shape=[
            in_hbm((rows, width), jnp.bfloat16),
            in_hbm((rows, LANES)),
            in_hbm((lines, 2, half)),
            in_hbm((2, half)),
        ],
        scratch_shapes=[
            pltpu.VMEM((rows, width), jnp.bfloat16),
            pltpu.VMEM((rows, LANES), jnp.float32),
            pltpu.VMEM((lines, 2, half), jnp.float32),
            pltpu.VMEM((2, half), jnp.float32),
            pltpu.SemaphoreType.DMA((3 * (lines // 8) + 1,)),
        ],
        compiler_params=pltpu.CompilerParams(vmem_limit_bytes=12 << 20),
        name="actions",
    )(noise, elite_idx, mine, stay(tie), *state)


def refit_body(parts_ref, own_ref, slice_ref, peak_ref, *, elites):
    total = jnp.sum(parts_ref[...], axis=0)
    mean = total[0:1] / elites
    variance = jnp.maximum(total[1:2] / elites - mean * mean, 0.0)
    slice_ref[0:1, :] = MOMENTUM * own_ref[0:1, :] + (1.0 - MOMENTUM) * mean
    mixed = MOMENTUM * own_ref[1:2, :] + (1.0 - MOMENTUM) * jnp.sqrt(variance)
    slice_ref[1:2, :] = mixed
    peak_ref[...] = jnp.broadcast_to(jnp.max(mixed, axis=1, keepdims=True)[None], peak_ref.shape)


def refit(parts, own, elites, groups):
    return pl.pallas_call(
        functools.partial(refit_body, elites=elites),
        in_specs=[VMEM, VMEM],
        out_specs=[VMEM, VMEM],
        out_shape=[
            jax.ShapeDtypeStruct(own.shape, jnp.float32),
            jax.ShapeDtypeStruct((groups, 1, LANES), jnp.float32),
        ],
        compiler_params=pltpu.CompilerParams(vmem_limit_bytes=4 << 20),
        name="refit",
    )(parts, own)


def spread_body(slice_ref, peak_ref, tie_ref, out_ref, token_ref):
    lines = out_ref.shape[0]
    half = slice_ref.shape[1]
    lane = lax.broadcasted_iota(jnp.int32, (1, LANES), 1)
    tail = jnp.zeros((1, LANES), jnp.float32)
    for group in range(peak_ref.shape[0]):
        tail = jnp.where(lane == group, peak_ref[group], tail)
    main = jnp.broadcast_to(slice_ref[...][None], (lines, 2, half))
    out_ref[:, :, pl.ds(0, half)] = main
    token_ref[...] = jnp.broadcast_to(tail, token_ref.shape)
    out_ref[:, :, pl.ds(half, LANES)] = jnp.broadcast_to(tail[None], (lines, 2, LANES))


def to_all(piece, peaks, tie, lines):
    half = piece.shape[1]
    return pl.pallas_call(
        spread_body,
        grid=(1,),
        in_specs=[VMEM, VMEM, HBM],
        out_specs=[whole((lines, 2, half + LANES)), whole((8, LANES))],
        out_shape=[in_hbm((lines, 2, half + LANES)), in_hbm((8, LANES))],
        compiler_params=pltpu.CompilerParams(vmem_limit_bytes=4 << 20),
        name="to_all",
    )(piece, peaks, stay(tie))


def final_body(state_ref, mean_ref, std_ref, *, envs_total):
    envs, width = mean_ref.shape
    half = width // 2
    floor, gain = stats_of(state_ref, envs, half, envs_total)
    for env in range(envs):
        for side in range(2):
            lanes = pl.ds(side * half, half)
            line = 2 * env + side
            mean_ref[pl.ds(env, 1), lanes] = state_ref[line, 0:1, pl.ds(0, half)]
            std_ref[pl.ds(env, 1), lanes] = (
                jnp.maximum(state_ref[line, 1:2, pl.ds(0, half)], floor) * gain
            )


def finished(state, envs, width, envs_total):
    shape = jax.ShapeDtypeStruct((envs, width), jnp.float32)
    return pl.pallas_call(
        functools.partial(final_body, envs_total=envs_total),
        in_specs=[VMEM],
        out_specs=[VMEM, VMEM],
        out_shape=[shape, shape],
        compiler_params=pltpu.CompilerParams(vmem_limit_bytes=4 << 20),
        name="finished",
    )(state)


def rollout_body(*refs, spans, act_dim, total, earlier, keep):
    refs = list(refs)
    take = lambda n: [refs.pop(0) for _ in range(n)]
    acts = take(len(spans))
    carried = [take(1)[0] if first else None for first, _ in spans]
    squares = [take(1)[0] if last == total else None for _, last in spans]
    begin_ref, goal_ref, ws_ref, wa_ref, wout_ref, bin_ref, bout_ref = take(7)
    before = take(earlier)
    tie_ref = take(1)[0]
    outs = take(len(spans))
    same_ref = take(1)[0] if keep else None
    moves, win, start, goal, square, sems = refs
    envs, dim = begin_ref.shape
    rows = acts[0].shape[0]
    cands = rows // envs
    steps = spans[0][1] - spans[0][0]
    copies = []
    for k, (first, last) in enumerate(spans):
        copies.append(
            pltpu.make_async_copy(
                acts[k].at[:, pl.ds(first * act_dim, steps * act_dim)],
                moves.at[pl.ds(k * rows, rows), :],
                sems.at[k],
            )
        )
    late = []
    number = iter(range(len(spans), SLOTS))
    for k, (_, last) in enumerate(spans):
        if carried[k] is not None:
            target = start.at[:, pl.ds(k * rows, rows), :]
            copies.append(pltpu.make_async_copy(carried[k], target, sems.at[next(number)]))
        if last == total:
            late.append(pltpu.make_async_copy(squares[k], square, sems.at[next(number)]))
            for n in range(earlier):
                late.append(
                    pltpu.make_async_copy(before[n].at[0], outs[k].at[n], sems.at[next(number)])
                )
    if keep:
        late.append(pltpu.make_async_copy(tie_ref, same_ref, sems.at[next(number)]))
    for copy in copies + late:
        copy.start()
    zeros = jnp.zeros(wa_ref.shape, jnp.bfloat16)
    for parity in range(2):
        win[parity, pl.ds(0, dim), :] = ws_ref[...] * jnp.bfloat16(0.5)
        win[parity, pl.ds(dim + parity * act_dim, act_dim), :] = wa_ref[...] * jnp.bfloat16(0.5)
        win[parity, pl.ds(dim + (1 - parity) * act_dim, act_dim), :] = zeros
    for k in range(len(spans)):
        for env in range(envs):
            at = pl.ds(k * rows + env * cands, cands)
            if carried[k] is None:
                start[0, at, :] = jnp.broadcast_to(begin_ref[pl.ds(env, 1), :], (cands, dim))
            goal[at, :] = jnp.broadcast_to(goal_ref[pl.ds(env, 1), :], (cands, dim))
        at = pl.ds(k * rows, rows)
        if carried[k] is None:
            start[1, at, :] = jnp.zeros((rows, dim), jnp.float32)
    bias_in = bin_ref[...] * 0.5
    for copy in copies:
        copy.wait()

    many = 4 if steps % 4 == 0 else 2

    def some_steps(k, carry):
        state, error = carry
        for n in range(many):
            parity = n % 2
            at = pl.multiple_of((k * many + n - parity) * act_dim, 2 * act_dim)
            pair = moves[:, pl.ds(at, 2 * act_dim)]
            joined = jnp.concatenate([state.astype(jnp.bfloat16), pair], axis=1)
            half = jnp.dot(joined, win[parity], preferred_element_type=jnp.float32) + bias_in
            hidden = (half + half * jnp.tanh(half)).astype(jnp.bfloat16)
            moved = jnp.dot(hidden, wout_ref[...], preferred_element_type=jnp.float32)
            state = jnp.tanh(state + moved + bout_ref[...])
            gap = state - goal[...]
            error = error + gap * gap
        return state, error

    state, error = lax.fori_loop(0, steps // many, some_steps, (start[0], start[1]))
    for copy in late:
        copy.wait()
    for k, (_, last) in enumerate(spans):
        part = slice(k * rows, (k + 1) * rows)
        if last < total:
            outs[k][0] = state[part]
            outs[k][1] = error[part]
            continue
        both = error[part] / (dim * total) + square[...] * (ACT_COST / (act_dim * total))
        cost = jnp.broadcast_to(jnp.sum(both, axis=1, keepdims=True), (rows, LANES))
        lane = lax.broadcasted_iota(jnp.int32, (cands, LANES), 1)
        table = jnp.zeros((cands, LANES), jnp.float32)
        for env in range(envs):
            table = jnp.where(lane == env, cost[env * cands : (env + 1) * cands], table)
        outs[k][earlier] = table[:, :envs]


def rollout(parts, fixed, before, tie, act_dim, keep):
    rows, width = parts[0][0].shape
    envs, dim = fixed[0].shape
    cands = rows // envs
    total = width // act_dim
    spans = [(p[3], p[4]) for p in parts]
    steps = spans[0][1] - spans[0][0]
    assert all(b - a == steps and a % 2 == 0 for a, b in spans) and steps % 2 == 0
    acts = [p[0] for p in parts]
    carried = [p[2] for p in parts if p[3]]
    squares = [p[1] for p in parts if p[4] == total]
    shapes = [
        (1 + len(before), cands, envs) if last == total else (2, rows, dim) for _, last in spans
    ]
    loose = carried + squares
    assert len(squares) <= 1
    return pl.pallas_call(
        functools.partial(
            rollout_body, spans=spans, act_dim=act_dim, total=total, earlier=len(before), keep=keep
        ),
        grid=(1,),
        in_specs=[HBM] * (len(acts) + len(loose))
        + [VMEM] * len(fixed)
        + [HBM] * (len(before) + 1),
        out_specs=[whole(shape) for shape in shapes] + [VMEM] * keep,
        out_shape=[in_hbm(shape) for shape in shapes]
        + [jax.ShapeDtypeStruct(tie.shape, tie.dtype)] * keep,
        scratch_shapes=[
            pltpu.VMEM((len(parts) * rows, steps * act_dim), jnp.bfloat16),
            pltpu.VMEM((2, dim + 2 * act_dim, fixed[2].shape[1]), jnp.bfloat16),
            pltpu.VMEM((2, len(parts) * rows, dim), jnp.float32),
            pltpu.VMEM((len(parts) * rows, dim), jnp.float32),
            pltpu.VMEM((rows, LANES), jnp.float32),
            pltpu.SemaphoreType.DMA((SLOTS,)),
        ],
        cost_estimate=pl.CostEstimate(flops=ROLL_FLOPS, bytes_accessed=1 << 20, transcendentals=0),
        compiler_params=pltpu.CompilerParams(vmem_limit_bytes=10 << 20),
        name="rollout",
    )(*map(stay, acts), *map(stay, loose), *fixed, *map(stay, before), stay(tie))


def shards(
    white,
    mean_init,
    std_init,
    init_state,
    goal_state,
    w_state,
    w_action,
    w_out,
    bias_in,
    bias_out,
    elite_idx,
):
    iters, envs, cands, flat = white.shape
    act_dim = w_action.shape[0]
    length = flat // act_dim
    width = mean_init.shape[1]
    horizon = width // act_dim
    half = width // 2
    elites = elite_idx.shape[2]
    groups = lax.axis_size("env")
    peers = lax.axis_size("cand")
    lines = 2 * envs
    envs_total = envs * groups
    rows = envs * cands
    assert lines == peers and rows % 16 == 0
    assert iters == 3 and horizon == 40
    mine = lax.axis_index("cand").astype(jnp.int32)[None]
    fixed = (init_state, goal_state, w_state, w_action, w_out, bias_in[None], bias_out[None])
    white = white.reshape(iters, rows, flat)
    elite_idx = jnp.swapaxes(elite_idx, 0, 1)
    mix = functools.partial(lax.all_to_all, axis_name="cand", split_axis=0, concat_axis=0, tiled=True)
    acts, asq, held, costs = {}, {}, {}, {}

    def part(it, first, last):
        return (acts[it], asq[it], held.get(it), first, last)

    def play(parts, tie, before=(), keep=False):
        outs = rollout([part(*p) for p in parts], fixed, before, tie, act_dim, keep)
        for (it, _, last), out in zip(parts, outs):
            if last < horizon:
                held[it] = out
            else:
                costs[it] = out
        return outs[-1] if keep else outs[0]

    (noise,) = noise_of(white, 0, 1, None, act_dim, horizon)
    state, tie = (mean_init, std_init), mine
    for it in range(iters):
        acts[it], asq[it], sums, own = actions_of(
            noise, max(it - 1, 0), elite_idx, mine, tie, state, it, envs_total, lines, half
        )
        parts = mix(sums)
        if it == 0:
            noise, own = noise_of(white, 1, iters - 1, own, act_dim, horizon)
        elif it == 1:
            own = play([(0, 14, 26), (1, 0, 12)], own, keep=True)
        else:
            own = play([(1, 26, horizon), (2, 0, 14)], own, keep=True)
        piece, peak = refit(parts, own, elites, groups)
        peaks = lax.all_to_all(peak, "env", 0, 0, tiled=True)
        tie = mine if it < iters - 1 else play([(2, 14, 20)], peak)
        spread, token = to_all(piece, peaks, tie, lines)
        state = (mix(spread),)
        if it == 0:
            tie = play([(0, 0, 14)], token)
        elif it == 1:
            tie = play([(0, 26, horizon), (1, 12, 26)], token)
        else:
            tie = play([(2, 20, horizon)], token, (costs[0], costs[1]))
    mean, std = finished(state[0], envs, width, envs_total)
    return (mean, std, jnp.swapaxes(costs[iters - 1], 1, 2))


def solution(mesh):
    in_specs = (
        P(None, "env", "cand", None),
        P("env", None),
        P("env", None),
        P("env", None),
        P("env", None),
        P(),
        P(),
        P(),
        P(),
        P(),
        P("env", None, None),
    )
    out_specs = (P("env", None), P("env", None), P(None, "env", "cand"))
    return jax.shard_map(shards, mesh=mesh, in_specs=in_specs, out_specs=out_specs, check_vma=False)
```

```python
import functools

import jax
import jax.numpy as jnp
import numpy as np
from jax import lax
from jax.experimental import pallas as pl
from jax.experimental.pallas import tpu as pltpu
from jax.sharding import PartitionSpec as P

BETA_EXP = 2.5
MOMENTUM = 0.1
FLOOR_SHARE = 0.1
ACT_COST = 0.1
LANES = 128
SLOTS = 8
ROLL_FLOPS = 1 << 28
VMEM = pl.BlockSpec(memory_space=pltpu.VMEM)
SMEM = pl.BlockSpec(memory_space=pltpu.SMEM)
HBM = pl.BlockSpec(memory_space=pltpu.HBM)


def whole(shape):
    return pl.BlockSpec(shape, lambda i: (0,) * len(shape))


def stay(array):
    return pltpu.with_memory_space_constraint(array, pltpu.HBM)


def in_hbm(shape, dtype=jnp.float32):
    return pltpu.HBM(shape, dtype)


def color_kernel(length):
    freqs = np.arange(length // 2 + 1)
    scale = (np.maximum(freqs, 1).astype(np.float32) / np.float32(length)) ** np.float32(-BETA_EXP / 2)
    kernel = np.fft.irfft(scale.astype(np.float64), n=length)
    kernel = kernel / np.sqrt(np.sum(kernel * kernel))
    return np.asarray(kernel, np.float32).astype(jnp.bfloat16).astype(np.float32)


def noise_body(*refs, act_dim, first, keep):
    white_ref, out_ref = refs[0], refs[1 + keep]
    rows_in, packed, fill, sems = refs[-4:]
    count, _, width = out_ref.shape
    flat = white_ref.shape[2]
    length = flat // act_dim
    group = act_dim // 2
    per = 256 // group
    part = length * group

    def fetch(one):
        return pltpu.make_async_copy(white_ref.at[first + one], rows_in.at[one], sems.at[one])

    for one in range(count):
        fetch(one).start()
    if keep:
        hand = pltpu.make_async_copy(refs[1], refs[3], sems.at[count])
        hand.start()
    kernel = color_kernel(length)
    row = lax.broadcasted_iota(jnp.int32, (group, 256), 0)
    hit = lax.broadcasted_iota(jnp.int32, (group, 256), 1) % group == row
    spot = lax.broadcasted_iota(jnp.int32, (1, 256), 1) // group

    def step_at(n):
        return n // 4 * 4 + (0, 2, 1, 3)[n % 4]

    for n in range(length):
        band = jnp.full((1, 256), float(kernel[-step_at(n) % length]), jnp.float32)
        for q in range(1, per):
            band = jnp.where(spot == q, float(kernel[(step_at(q) - step_at(n)) % length]), band)
        tile = jnp.where(hit, band, 0.0).astype(jnp.bfloat16)
        fill[pl.ds(n * group, group), :] = tile
        fill[pl.ds(part + n * group, group), :] = tile
    even = lax.broadcasted_iota(jnp.int32, (1, LANES), 1) // group % 2 == 0

    def swap(a, b):
        low = jnp.where(even, a, pltpu.roll(b, group, 1))
        return low, jnp.where(even, pltpu.roll(a, LANES - group, 1), b)

    for one in range(count):
        fetch(one).wait()
        for k in range(flat // 256):
            pair = [
                rows_in[one, :, pl.ds(k * 256 + side * LANES, LANES)].astype(jnp.float32)
                for side in range(2)
            ]
            for side, piece in enumerate(swap(*pair)):
                packed[side, :, pl.ds(k * LANES, LANES)] = piece.astype(jnp.bfloat16)
        for block in range(width // (per * act_dim)):
            weights = fill[pl.ds((part - block * 256) % part, part), :]
            sides = [
                jnp.dot(packed[side], weights, preferred_element_type=jnp.float32)
                for side in range(2)
            ]
            for h in range(2):
                pair = [side[:, h * LANES : (h + 1) * LANES] for side in sides]
                at = block * 512 + h * 256
                for side, piece in enumerate(swap(*pair)):
                    out_ref[one, :, pl.ds(at + side * LANES, LANES)] = piece
    if keep:
        hand.wait()


def noise_of(white, first, count, own, act_dim, horizon):
    _, rows, flat = white.shape
    width = horizon * act_dim
    keep = own is not None
    assert act_dim == 64 and horizon % 8 == 0
    shapes = [jax.ShapeDtypeStruct((count, rows, width), jnp.float32)]
    if keep:
        shapes.append(jax.ShapeDtypeStruct(own.shape, own.dtype))
    return pl.pallas_call(
        functools.partial(noise_body, act_dim=act_dim, first=first, keep=keep),
        in_specs=[HBM] * (1 + keep),
        out_specs=[VMEM] * (1 + keep),
        out_shape=shapes,
        scratch_shapes=[
            pltpu.VMEM((count, rows, flat), jnp.bfloat16),
            pltpu.VMEM((2, rows, flat // 2), jnp.bfloat16),
            pltpu.VMEM((flat, 256), jnp.bfloat16),
            pltpu.SemaphoreType.DMA((count + 1,)),
        ],
        cost_estimate=pl.CostEstimate(flops=ROLL_FLOPS, bytes_accessed=1 << 20, transcendentals=0),
        compiler_params=pltpu.CompilerParams(vmem_limit_bytes=16 << 20),
        name="noise",
    )(stay(white), *([stay(own)] if keep else []))


def stats_of(state_ref, envs, half, envs_total):
    peaks = state_ref[:, 0, pl.ds(half, LANES)]
    pair = jnp.max(peaks.reshape(envs, 2, LANES), axis=1)
    peak = jnp.max(pair, axis=(0, 1), keepdims=True)
    total = jnp.sum(jnp.sum(pair, axis=0, keepdims=True), axis=1, keepdims=True)
    return FLOOR_SHARE * peak, 0.5 + total / (peak * envs_total)


def action_body(*refs, it, envs_total):
    first = it == 0
    if first:
        noise_ref, elite_ref, mine_ref, tie_ref, mean_ref, std_ref = refs[:6]
    else:
        noise_ref, elite_ref, mine_ref, tie_ref, state_ref = refs[:5]
    acts_out, asq_out, sums_out, own_out, acts_ref, asq_ref, sums_ref, own_ref, sems = refs[-9:]
    half = sums_ref.shape[2]
    rows = acts_ref.shape[0]
    envs = sums_ref.shape[0] // 2
    cands = rows // envs
    me = mine_ref[0]
    if first:
        lanes = pl.ds(pl.multiple_of((me % 2) * half, LANES), half)
        own_ref[0:1, :] = mean_ref[pl.ds(me // 2, 1), lanes]
        own_ref[1:2, :] = std_ref[pl.ds(me // 2, 1), lanes]
    else:
        floor, gain = stats_of(state_ref, envs, half, envs_total)
        own = state_ref[me, :, pl.ds(0, half)]
        own_ref[0:1, :] = own[0:1]
        own_ref[1:2, :] = jnp.maximum(own[1:2], floor) * gain
    per = 4

    def send(part):
        at = pl.ds(part * per * cands, per * cands)
        pair = pl.ds(part * per * 2, per * 2)
        trio = ((acts_ref, acts_out, at), (asq_ref, asq_out, at), (sums_ref, sums_out, pair))
        return [
            pltpu.make_async_copy(source.at[rows], target.at[rows], sems.at[3 * part + k])
            for k, (source, target, rows) in enumerate(trio)
        ]

    def send_own():
        return pltpu.make_async_copy(own_ref, own_out, sems.at[3 * (envs // per)])

    send_own().start()

    ids = me * cands + lax.broadcasted_iota(jnp.int32, (cands, 1), 0)
    for env in range(envs):
        at = pl.ds(env * cands, cands)
        chosen = elite_ref[it, env : env + 1, :] == ids
        member = jnp.sum(jnp.where(chosen, 1.0, 0.0), axis=1, keepdims=True)
        member = jnp.broadcast_to(member, (cands, LANES))
        square = jnp.zeros((cands, LANES), jnp.float32)
        for side in range(2):
            line = 2 * env + side
            for step in range(half // LANES):
                lanes = pl.ds(step * LANES, LANES)
                whole = pl.ds(side * half + step * LANES, LANES)
                if first:
                    center = mean_ref[pl.ds(env, 1), whole]
                    spread = std_ref[pl.ds(env, 1), whole]
                else:
                    center = state_ref[line, 0:1, lanes]
                    spread = jnp.maximum(state_ref[line, 1:2, lanes], floor) * gain
                action = jnp.clip(center + spread * noise_ref[0, at, whole], -1.0, 1.0)
                acts_ref[at, whole] = action.astype(jnp.bfloat16)
                both = action * action
                square = square + both
                sums_ref[line, 0:1, lanes] = jnp.sum(action * member, axis=0, keepdims=True)
                sums_ref[line, 1:2, lanes] = jnp.sum(both * member, axis=0, keepdims=True)
        asq_ref[at, :] = square
        if env % per == per - 1:
            for copy in send(env // per):
                copy.start()
    for part in range(envs // per):
        for copy in send(part):
            copy.wait()
    send_own().wait()


def actions_of(noise, at, elite_idx, mine, tie, state, it, envs_total, lines, half):
    _, rows, width = noise.shape
    return pl.pallas_call(
        functools.partial(action_body, it=it, envs_total=envs_total),
        grid=(1,),
        in_specs=[pl.BlockSpec((1, rows, width), lambda i: (at, 0, 0)), VMEM, SMEM, HBM]
        + [VMEM] * len(state),
        out_specs=[HBM] * 4,
        out_shape=[
            in_hbm((rows, width), jnp.bfloat16),
            in_hbm((rows, LANES)),
            in_hbm((lines, 2, half)),
            in_hbm((2, half)),
        ],
        scratch_shapes=[
            pltpu.VMEM((rows, width), jnp.bfloat16),
            pltpu.VMEM((rows, LANES), jnp.float32),
            pltpu.VMEM((lines, 2, half), jnp.float32),
            pltpu.VMEM((2, half), jnp.float32),
            pltpu.SemaphoreType.DMA((3 * (lines // 8) + 1,)),
        ],
        compiler_params=pltpu.CompilerParams(vmem_limit_bytes=12 << 20),
        name="actions",
    )(noise, elite_idx, mine, stay(tie), *state)


def refit_body(parts_ref, own_ref, slice_ref, peak_ref, *, elites):
    total = jnp.sum(parts_ref[...], axis=0)
    mean = total[0:1] / elites
    variance = jnp.maximum(total[1:2] / elites - mean * mean, 0.0)
    slice_ref[0:1, :] = MOMENTUM * own_ref[0:1, :] + (1.0 - MOMENTUM) * mean
    mixed = MOMENTUM * own_ref[1:2, :] + (1.0 - MOMENTUM) * jnp.sqrt(variance)
    slice_ref[1:2, :] = mixed
    peak_ref[...] = jnp.broadcast_to(jnp.max(mixed, axis=1, keepdims=True)[None], peak_ref.shape)


def refit(parts, own, elites, groups):
    return pl.pallas_call(
        functools.partial(refit_body, elites=elites),
        in_specs=[VMEM, VMEM],
        out_specs=[VMEM, VMEM],
        out_shape=[
            jax.ShapeDtypeStruct(own.shape, jnp.float32),
            jax.ShapeDtypeStruct((groups, 1, LANES), jnp.float32),
        ],
        compiler_params=pltpu.CompilerParams(vmem_limit_bytes=4 << 20),
        name="refit",
    )(parts, own)


def spread_body(slice_ref, peak_ref, tie_ref, out_ref, token_ref):
    lines = out_ref.shape[0]
    half = slice_ref.shape[1]
    lane = lax.broadcasted_iota(jnp.int32, (1, LANES), 1)
    tail = jnp.zeros((1, LANES), jnp.float32)
    for group in range(peak_ref.shape[0]):
        tail = jnp.where(lane == group, peak_ref[group], tail)
    main = jnp.broadcast_to(slice_ref[...][None], (lines, 2, half))
    out_ref[:, :, pl.ds(0, half)] = main
    token_ref[...] = jnp.broadcast_to(tail, token_ref.shape)
    out_ref[:, :, pl.ds(half, LANES)] = jnp.broadcast_to(tail[None], (lines, 2, LANES))


def to_all(piece, peaks, tie, lines):
    half = piece.shape[1]
    return pl.pallas_call(
        spread_body,
        grid=(1,),
        in_specs=[VMEM, VMEM, HBM],
        out_specs=[whole((lines, 2, half + LANES)), whole((8, LANES))],
        out_shape=[in_hbm((lines, 2, half + LANES)), in_hbm((8, LANES))],
        compiler_params=pltpu.CompilerParams(vmem_limit_bytes=4 << 20),
        name="to_all",
    )(piece, peaks, stay(tie))


def final_body(state_ref, mean_ref, std_ref, *, envs_total):
    envs, width = mean_ref.shape
    half = width // 2
    floor, gain = stats_of(state_ref, envs, half, envs_total)
    for env in range(envs):
        for side in range(2):
            lanes = pl.ds(side * half, half)
            line = 2 * env + side
            mean_ref[pl.ds(env, 1), lanes] = state_ref[line, 0:1, pl.ds(0, half)]
            std_ref[pl.ds(env, 1), lanes] = (
                jnp.maximum(state_ref[line, 1:2, pl.ds(0, half)], floor) * gain
            )


def finished(state, envs, width, envs_total):
    shape = jax.ShapeDtypeStruct((envs, width), jnp.float32)
    return pl.pallas_call(
        functools.partial(final_body, envs_total=envs_total),
        in_specs=[VMEM],
        out_specs=[VMEM, VMEM],
        out_shape=[shape, shape],
        compiler_params=pltpu.CompilerParams(vmem_limit_bytes=4 << 20),
        name="finished",
    )(state)


def rollout_body(*refs, spans, act_dim, total, earlier, keep):
    refs = list(refs)
    take = lambda n: [refs.pop(0) for _ in range(n)]
    acts = take(len(spans))
    carried = [take(1)[0] if first else None for first, _ in spans]
    squares = [take(1)[0] if last == total else None for _, last in spans]
    begin_ref, goal_ref, ws_ref, wa_ref, wout_ref, bin_ref, bout_ref = take(7)
    before = take(earlier)
    tie_ref = take(1)[0]
    outs = take(len(spans))
    same_ref = take(1)[0] if keep else None
    moves, win, start, goal, square, sems = refs
    envs, dim = begin_ref.shape
    rows = acts[0].shape[0]
    cands = rows // envs
    steps = spans[0][1] - spans[0][0]
    copies = []
    for k, (first, last) in enumerate(spans):
        copies.append(
            pltpu.make_async_copy(
                acts[k].at[:, pl.ds(first * act_dim, steps * act_dim)],
                moves.at[pl.ds(k * rows, rows), :],
                sems.at[k],
            )
        )
    late = []
    number = iter(range(len(spans), SLOTS))
    for k, (_, last) in enumerate(spans):
        if carried[k] is not None:
            target = start.at[:, pl.ds(k * rows, rows), :]
            copies.append(pltpu.make_async_copy(carried[k], target, sems.at[next(number)]))
        if last == total:
            late.append(pltpu.make_async_copy(squares[k], square, sems.at[next(number)]))
            for n in range(earlier):
                late.append(
                    pltpu.make_async_copy(before[n].at[0], outs[k].at[n], sems.at[next(number)])
                )
    if keep:
        late.append(pltpu.make_async_copy(tie_ref, same_ref, sems.at[next(number)]))
    for copy in copies + late:
        copy.start()
    zeros = jnp.zeros(wa_ref.shape, jnp.bfloat16)
    for parity in range(2):
        win[parity, pl.ds(0, dim), :] = ws_ref[...] * jnp.bfloat16(0.5)
        win[parity, pl.ds(dim + parity * act_dim, act_dim), :] = wa_ref[...] * jnp.bfloat16(0.5)
        win[parity, pl.ds(dim + (1 - parity) * act_dim, act_dim), :] = zeros
    for k in range(len(spans)):
        for env in range(envs):
            at = pl.ds(k * rows + env * cands, cands)
            if carried[k] is None:
                start[0, at, :] = jnp.broadcast_to(begin_ref[pl.ds(env, 1), :], (cands, dim))
            goal[at, :] = jnp.broadcast_to(goal_ref[pl.ds(env, 1), :], (cands, dim))
        at = pl.ds(k * rows, rows)
        if carried[k] is None:
            start[1, at, :] = jnp.zeros((rows, dim), jnp.float32)
    bias_in = bin_ref[...] * 0.5
    for copy in copies:
        copy.wait()

    many = 4 if steps % 4 == 0 else 2

    def some_steps(k, carry):
        state, error = carry
        for n in range(many):
            parity = n % 2
            at = pl.multiple_of((k * many + n - parity) * act_dim, 2 * act_dim)
            pair = moves[:, pl.ds(at, 2 * act_dim)]
            joined = jnp.concatenate([state.astype(jnp.bfloat16), pair], axis=1)
            half = jnp.dot(joined, win[parity], preferred_element_type=jnp.float32) + bias_in
            hidden = (half + half * jnp.tanh(half)).astype(jnp.bfloat16)
            moved = jnp.dot(hidden, wout_ref[...], preferred_element_type=jnp.float32)
            state = jnp.tanh(state + moved + bout_ref[...])
            gap = state - goal[...]
            error = error + gap * gap
        return state, error

    state, error = lax.fori_loop(0, steps // many, some_steps, (start[0], start[1]))
    for copy in late:
        copy.wait()
    for k, (_, last) in enumerate(spans):
        part = slice(k * rows, (k + 1) * rows)
        if last < total:
            outs[k][0] = state[part]
            outs[k][1] = error[part]
            continue
        both = error[part] / (dim * total) + square[...] * (ACT_COST / (act_dim * total))
        cost = jnp.broadcast_to(jnp.sum(both, axis=1, keepdims=True), (rows, LANES))
        lane = lax.broadcasted_iota(jnp.int32, (cands, LANES), 1)
        table = jnp.zeros((cands, LANES), jnp.float32)
        for env in range(envs):
            table = jnp.where(lane == env, cost[env * cands : (env + 1) * cands], table)
        outs[k][earlier] = table[:, :envs]


def rollout(parts, fixed, before, tie, act_dim, keep):
    rows, width = parts[0][0].shape
    envs, dim = fixed[0].shape
    cands = rows // envs
    total = width // act_dim
    spans = [(p[3], p[4]) for p in parts]
    steps = spans[0][1] - spans[0][0]
    assert all(b - a == steps and a % 2 == 0 for a, b in spans) and steps % 2 == 0
    acts = [p[0] for p in parts]
    carried = [p[2] for p in parts if p[3]]
    squares = [p[1] for p in parts if p[4] == total]
    shapes = [
        (1 + len(before), cands, envs) if last == total else (2, rows, dim) for _, last in spans
    ]
    loose = carried + squares
    assert len(squares) <= 1
    return pl.pallas_call(
        functools.partial(
            rollout_body, spans=spans, act_dim=act_dim, total=total, earlier=len(before), keep=keep
        ),
        grid=(1,),
        in_specs=[HBM] * (len(acts) + len(loose))
        + [VMEM] * len(fixed)
        + [HBM] * (len(before) + 1),
        out_specs=[whole(shape) for shape in shapes] + [VMEM] * keep,
        out_shape=[in_hbm(shape) for shape in shapes]
        + [jax.ShapeDtypeStruct(tie.shape, tie.dtype)] * keep,
        scratch_shapes=[
            pltpu.VMEM((len(parts) * rows, steps * act_dim), jnp.bfloat16),
            pltpu.VMEM((2, dim + 2 * act_dim, fixed[2].shape[1]), jnp.bfloat16),
            pltpu.VMEM((2, len(parts) * rows, dim), jnp.float32),
            pltpu.VMEM((len(parts) * rows, dim), jnp.float32),
            pltpu.VMEM((rows, LANES), jnp.float32),
            pltpu.SemaphoreType.DMA((SLOTS,)),
        ],
        cost_estimate=pl.CostEstimate(flops=ROLL_FLOPS, bytes_accessed=1 << 20, transcendentals=0),
        compiler_params=pltpu.CompilerParams(vmem_limit_bytes=10 << 20),
        name="rollout",
    )(*map(stay, acts), *map(stay, loose), *fixed, *map(stay, before), stay(tie))


def shards(
    white,
    mean_init,
    std_init,
    init_state,
    goal_state,
    w_state,
    w_action,
    w_out,
    bias_in,
    bias_out,
    elite_idx,
):
    iters, envs, cands, flat = white.shape
    act_dim = w_action.shape[0]
    length = flat // act_dim
    width = mean_init.shape[1]
    horizon = width // act_dim
    half = width // 2
    elites = elite_idx.shape[2]
    groups = lax.axis_size("env")
    peers = lax.axis_size("cand")
    lines = 2 * envs
    envs_total = envs * groups
    rows = envs * cands
    assert lines == peers and rows % 16 == 0
    assert iters == 3 and horizon == 40
    mine = lax.axis_index("cand").astype(jnp.int32)[None]
    fixed = (init_state, goal_state, w_state, w_action, w_out, bias_in[None], bias_out[None])
    white = white.reshape(iters, rows, flat)
    elite_idx = jnp.swapaxes(elite_idx, 0, 1)
    mix = functools.partial(lax.all_to_all, axis_name="cand", split_axis=0, concat_axis=0, tiled=True)
    acts, asq, held, costs = {}, {}, {}, {}

    def part(it, first, last):
        return (acts[it], asq[it], held.get(it), first, last)

    def play(parts, tie, before=(), keep=False):
        outs = rollout([part(*p) for p in parts], fixed, before, tie, act_dim, keep)
        for (it, _, last), out in zip(parts, outs):
            if last < horizon:
                held[it] = out
            else:
                costs[it] = out
        return outs[-1] if keep else outs[0]

    (noise,) = noise_of(white, 0, 1, None, act_dim, horizon)
    state, tie = (mean_init, std_init), mine
    for it in range(iters):
        acts[it], asq[it], sums, own = actions_of(
            noise, max(it - 1, 0), elite_idx, mine, tie, state, it, envs_total, lines, half
        )
        parts = mix(sums)
        if it == 0:
            noise, own = noise_of(white, 1, iters - 1, own, act_dim, horizon)
        elif it == 1:
            own = play([(0, 14, 28), (1, 0, 14)], own, keep=True)
        else:
            own = play([(1, 26, horizon), (2, 0, 14)], own, keep=True)
        piece, peak = refit(parts, own, elites, groups)
        peaks = lax.all_to_all(peak, "env", 0, 0, tiled=True)
        tie = mine if it < iters - 1 else play([(2, 14, 20)], peak)
        spread, token = to_all(piece, peaks, tie, lines)
        state = (mix(spread),)
        if it == 0:
            tie = play([(0, 0, 14)], token)
        elif it == 1:
            tie = play([(0, 28, horizon), (1, 14, 26)], token)
        else:
            tie = play([(2, 20, horizon)], token, (costs[0], costs[1]))
    mean, std = finished(state[0], envs, width, envs_total)
    return (mean, std, jnp.swapaxes(costs[iters - 1], 1, 2))


def solution(mesh):
    in_specs = (
        P(None, "env", "cand", None),
        P("env", None),
        P("env", None),
        P("env", None),
        P("env", None),
        P(),
        P(),
        P(),
        P(),
        P(),
        P("env", None, None),
    )
    out_specs = (P("env", None), P("env", None), P(None, "env", "cand"))
    return jax.shard_map(shards, mesh=mesh, in_specs=in_specs, out_specs=out_specs, check_vma=False)
```

```python
import functools

import jax
import jax.numpy as jnp
import numpy as np
from jax import lax
from jax.experimental import pallas as pl
from jax.experimental.pallas import tpu as pltpu
from jax.sharding import PartitionSpec as P

BETA_EXP = 2.5
MOMENTUM = 0.1
FLOOR_SHARE = 0.1
ACT_COST = 0.1
LANES = 128
SLOTS = 8
ROLL_FLOPS = 1 << 28
VMEM = pl.BlockSpec(memory_space=pltpu.VMEM)
SMEM = pl.BlockSpec(memory_space=pltpu.SMEM)
HBM = pl.BlockSpec(memory_space=pltpu.HBM)


def whole(shape):
    return pl.BlockSpec(shape, lambda i: (0,) * len(shape))


def stay(array):
    return pltpu.with_memory_space_constraint(array, pltpu.HBM)


def in_hbm(shape, dtype=jnp.float32):
    return pltpu.HBM(shape, dtype)


def color_kernel(length):
    freqs = np.arange(length // 2 + 1)
    scale = (np.maximum(freqs, 1).astype(np.float32) / np.float32(length)) ** np.float32(-BETA_EXP / 2)
    kernel = np.fft.irfft(scale.astype(np.float64), n=length)
    kernel = kernel / np.sqrt(np.sum(kernel * kernel))
    return np.asarray(kernel, np.float32).astype(jnp.bfloat16).astype(np.float32)


def noise_body(*refs, act_dim, first, keep):
    white_ref, out_ref = refs[0], refs[1 + keep]
    rows_in, packed, fill, sems = refs[-4:]
    count, _, width = out_ref.shape
    flat = white_ref.shape[2]
    length = flat // act_dim
    group = act_dim // 2
    per = 256 // group
    part = length * group

    def fetch(one):
        return pltpu.make_async_copy(white_ref.at[first + one], rows_in.at[one], sems.at[one])

    for one in range(count):
        fetch(one).start()
    if keep:
        hand = pltpu.make_async_copy(refs[1], refs[3], sems.at[count])
        hand.start()
    kernel = color_kernel(length)
    row = lax.broadcasted_iota(jnp.int32, (group, 256), 0)
    hit = lax.broadcasted_iota(jnp.int32, (group, 256), 1) % group == row
    spot = lax.broadcasted_iota(jnp.int32, (1, 256), 1) // group

    def step_at(n):
        return n // 4 * 4 + (0, 2, 1, 3)[n % 4]

    for n in range(length):
        band = jnp.full((1, 256), float(kernel[-step_at(n) % length]), jnp.float32)
        for q in range(1, per):
            band = jnp.where(spot == q, float(kernel[(step_at(q) - step_at(n)) % length]), band)
        tile = jnp.where(hit, band, 0.0).astype(jnp.bfloat16)
        fill[pl.ds(n * group, group), :] = tile
        fill[pl.ds(part + n * group, group), :] = tile
    even = lax.broadcasted_iota(jnp.int32, (1, LANES), 1) // group % 2 == 0

    def swap(a, b):
        low = jnp.where(even, a, pltpu.roll(b, group, 1))
        return low, jnp.where(even, pltpu.roll(a, LANES - group, 1), b)

    for one in range(count):
        fetch(one).wait()
        for k in range(flat // 256):
            pair = [
                rows_in[one, :, pl.ds(k * 256 + side * LANES, LANES)].astype(jnp.float32)
                for side in range(2)
            ]
            for side, piece in enumerate(swap(*pair)):
                packed[side, :, pl.ds(k * LANES, LANES)] = piece.astype(jnp.bfloat16)
        for block in range(width // (per * act_dim)):
            weights = fill[pl.ds((part - block * 256) % part, part), :]
            sides = [
                jnp.dot(packed[side], weights, preferred_element_type=jnp.float32)
                for side in range(2)
            ]
            for h in range(2):
                pair = [side[:, h * LANES : (h + 1) * LANES] for side in sides]
                at = block * 512 + h * 256
                for side, piece in enumerate(swap(*pair)):
                    out_ref[one, :, pl.ds(at + side * LANES, LANES)] = piece
    if keep:
        hand.wait()


def noise_of(white, first, count, own, act_dim, horizon):
    _, rows, flat = white.shape
    width = horizon * act_dim
    keep = own is not None
    assert act_dim == 64 and horizon % 8 == 0
    shapes = [jax.ShapeDtypeStruct((count, rows, width), jnp.float32)]
    if keep:
        shapes.append(jax.ShapeDtypeStruct(own.shape, own.dtype))
    return pl.pallas_call(
        functools.partial(noise_body, act_dim=act_dim, first=first, keep=keep),
        in_specs=[HBM] * (1 + keep),
        out_specs=[VMEM] * (1 + keep),
        out_shape=shapes,
        scratch_shapes=[
            pltpu.VMEM((count, rows, flat), jnp.bfloat16),
            pltpu.VMEM((2, rows, flat // 2), jnp.bfloat16),
            pltpu.VMEM((flat, 256), jnp.bfloat16),
            pltpu.SemaphoreType.DMA((count + 1,)),
        ],
        cost_estimate=pl.CostEstimate(flops=ROLL_FLOPS, bytes_accessed=1 << 20, transcendentals=0),
        compiler_params=pltpu.CompilerParams(vmem_limit_bytes=16 << 20),
        name="noise",
    )(stay(white), *([stay(own)] if keep else []))


def stats_of(state_ref, envs, half, envs_total):
    peaks = state_ref[:, 0, pl.ds(half, LANES)]
    pair = jnp.max(peaks.reshape(envs, 2, LANES), axis=1)
    peak = jnp.max(pair, axis=(0, 1), keepdims=True)
    total = jnp.sum(jnp.sum(pair, axis=0, keepdims=True), axis=1, keepdims=True)
    return FLOOR_SHARE * peak, 0.5 + total / (peak * envs_total)


def action_body(*refs, it, envs_total):
    first = it == 0
    if first:
        noise_ref, elite_ref, mine_ref, tie_ref, mean_ref, std_ref = refs[:6]
    else:
        noise_ref, elite_ref, mine_ref, tie_ref, state_ref = refs[:5]
    acts_out, asq_out, sums_out, own_out, acts_ref, asq_ref, sums_ref, own_ref, sems = refs[-9:]
    half = sums_ref.shape[2]
    rows = acts_ref.shape[0]
    envs = sums_ref.shape[0] // 2
    cands = rows // envs
    me = mine_ref[0]
    if first:
        lanes = pl.ds(pl.multiple_of((me % 2) * half, LANES), half)
        own_ref[0:1, :] = mean_ref[pl.ds(me // 2, 1), lanes]
        own_ref[1:2, :] = std_ref[pl.ds(me // 2, 1), lanes]
    else:
        floor, gain = stats_of(state_ref, envs, half, envs_total)
        own = state_ref[me, :, pl.ds(0, half)]
        own_ref[0:1, :] = own[0:1]
        own_ref[1:2, :] = jnp.maximum(own[1:2], floor) * gain
    per = 4

    def send(part):
        at = pl.ds(part * per * cands, per * cands)
        pair = pl.ds(part * per * 2, per * 2)
        trio = ((acts_ref, acts_out, at), (asq_ref, asq_out, at), (sums_ref, sums_out, pair))
        return [
            pltpu.make_async_copy(source.at[rows], target.at[rows], sems.at[3 * part + k])
            for k, (source, target, rows) in enumerate(trio)
        ]

    def send_own():
        return pltpu.make_async_copy(own_ref, own_out, sems.at[3 * (envs // per)])

    send_own().start()

    ids = me * cands + lax.broadcasted_iota(jnp.int32, (cands, 1), 0)
    for env in range(envs):
        at = pl.ds(env * cands, cands)
        chosen = elite_ref[it, env : env + 1, :] == ids
        member = jnp.sum(jnp.where(chosen, 1.0, 0.0), axis=1, keepdims=True)
        member = jnp.broadcast_to(member, (cands, LANES))
        square = jnp.zeros((cands, LANES), jnp.float32)
        for side in range(2):
            line = 2 * env + side
            for step in range(half // LANES):
                lanes = pl.ds(step * LANES, LANES)
                whole = pl.ds(side * half + step * LANES, LANES)
                if first:
                    center = mean_ref[pl.ds(env, 1), whole]
                    spread = std_ref[pl.ds(env, 1), whole]
                else:
                    center = state_ref[line, 0:1, lanes]
                    spread = jnp.maximum(state_ref[line, 1:2, lanes], floor) * gain
                action = jnp.clip(center + spread * noise_ref[0, at, whole], -1.0, 1.0)
                acts_ref[at, whole] = action.astype(jnp.bfloat16)
                both = action * action
                square = square + both
                sums_ref[line, 0:1, lanes] = jnp.sum(action * member, axis=0, keepdims=True)
                sums_ref[line, 1:2, lanes] = jnp.sum(both * member, axis=0, keepdims=True)
        asq_ref[at, :] = square
        if env % per == per - 1:
            for copy in send(env // per):
                copy.start()
    for part in range(envs // per):
        for copy in send(part):
            copy.wait()
    send_own().wait()


def actions_of(noise, at, elite_idx, mine, tie, state, it, envs_total, lines, half):
    _, rows, width = noise.shape
    return pl.pallas_call(
        functools.partial(action_body, it=it, envs_total=envs_total),
        grid=(1,),
        in_specs=[pl.BlockSpec((1, rows, width), lambda i: (at, 0, 0)), VMEM, SMEM, HBM]
        + [VMEM] * len(state),
        out_specs=[HBM] * 4,
        out_shape=[
            in_hbm((rows, width), jnp.bfloat16),
            in_hbm((rows, LANES)),
            in_hbm((lines, 2, half)),
            in_hbm((2, half)),
        ],
        scratch_shapes=[
            pltpu.VMEM((rows, width), jnp.bfloat16),
            pltpu.VMEM((rows, LANES), jnp.float32),
            pltpu.VMEM((lines, 2, half), jnp.float32),
            pltpu.VMEM((2, half), jnp.float32),
            pltpu.SemaphoreType.DMA((3 * (lines // 8) + 1,)),
        ],
        compiler_params=pltpu.CompilerParams(vmem_limit_bytes=12 << 20),
        name="actions",
    )(noise, elite_idx, mine, stay(tie), *state)


def refit_body(parts_ref, own_ref, slice_ref, peak_ref, *, elites):
    total = jnp.sum(parts_ref[...], axis=0)
    mean = total[0:1] / elites
    variance = jnp.maximum(total[1:2] / elites - mean * mean, 0.0)
    slice_ref[0:1, :] = MOMENTUM * own_ref[0:1, :] + (1.0 - MOMENTUM) * mean
    mixed = MOMENTUM * own_ref[1:2, :] + (1.0 - MOMENTUM) * jnp.sqrt(variance)
    slice_ref[1:2, :] = mixed
    peak_ref[...] = jnp.broadcast_to(jnp.max(mixed, axis=1, keepdims=True)[None], peak_ref.shape)


def refit(parts, own, elites, groups):
    return pl.pallas_call(
        functools.partial(refit_body, elites=elites),
        in_specs=[VMEM, VMEM],
        out_specs=[VMEM, VMEM],
        out_shape=[
            jax.ShapeDtypeStruct(own.shape, jnp.float32),
            jax.ShapeDtypeStruct((groups, 1, LANES), jnp.float32),
        ],
        compiler_params=pltpu.CompilerParams(vmem_limit_bytes=4 << 20),
        name="refit",
    )(parts, own)


def spread_body(slice_ref, peak_ref, tie_ref, out_ref, token_ref):
    lines = out_ref.shape[0]
    half = slice_ref.shape[1]
    lane = lax.broadcasted_iota(jnp.int32, (1, LANES), 1)
    tail = jnp.zeros((1, LANES), jnp.float32)
    for group in range(peak_ref.shape[0]):
        tail = jnp.where(lane == group, peak_ref[group], tail)
    main = jnp.broadcast_to(slice_ref[...][None], (lines, 2, half))
    out_ref[:, :, pl.ds(0, half)] = main
    token_ref[...] = jnp.broadcast_to(tail, token_ref.shape)
    out_ref[:, :, pl.ds(half, LANES)] = jnp.broadcast_to(tail[None], (lines, 2, LANES))


def to_all(piece, peaks, tie, lines):
    half = piece.shape[1]
    return pl.pallas_call(
        spread_body,
        grid=(1,),
        in_specs=[VMEM, VMEM, HBM],
        out_specs=[whole((lines, 2, half + LANES)), whole((8, LANES))],
        out_shape=[in_hbm((lines, 2, half + LANES)), in_hbm((8, LANES))],
        compiler_params=pltpu.CompilerParams(vmem_limit_bytes=4 << 20),
        name="to_all",
    )(piece, peaks, stay(tie))


def final_body(state_ref, mean_ref, std_ref, *, envs_total):
    envs, width = mean_ref.shape
    half = width // 2
    floor, gain = stats_of(state_ref, envs, half, envs_total)
    for env in range(envs):
        for side in range(2):
            lanes = pl.ds(side * half, half)
            line = 2 * env + side
            mean_ref[pl.ds(env, 1), lanes] = state_ref[line, 0:1, pl.ds(0, half)]
            std_ref[pl.ds(env, 1), lanes] = (
                jnp.maximum(state_ref[line, 1:2, pl.ds(0, half)], floor) * gain
            )


def finished(state, envs, width, envs_total):
    shape = jax.ShapeDtypeStruct((envs, width), jnp.float32)
    return pl.pallas_call(
        functools.partial(final_body, envs_total=envs_total),
        in_specs=[VMEM],
        out_specs=[VMEM, VMEM],
        out_shape=[shape, shape],
        compiler_params=pltpu.CompilerParams(vmem_limit_bytes=4 << 20),
        name="finished",
    )(state)


def rollout_body(*refs, spans, act_dim, total, earlier, keep):
    refs = list(refs)
    take = lambda n: [refs.pop(0) for _ in range(n)]
    acts = take(len(spans))
    carried = [take(1)[0] if first else None for first, _ in spans]
    squares = [take(1)[0] if last == total else None for _, last in spans]
    begin_ref, goal_ref, ws_ref, wa_ref, wout_ref, bin_ref, bout_ref = take(7)
    before = take(earlier)
    tie_ref = take(1)[0]
    outs = take(len(spans))
    same_ref = take(1)[0] if keep else None
    moves, win, start, goal, square, sems = refs
    envs, dim = begin_ref.shape
    rows = acts[0].shape[0]
    cands = rows // envs
    steps = spans[0][1] - spans[0][0]
    copies = []
    for k, (first, last) in enumerate(spans):
        copies.append(
            pltpu.make_async_copy(
                acts[k].at[:, pl.ds(first * act_dim, steps * act_dim)],
                moves.at[pl.ds(k * rows, rows), :],
                sems.at[k],
            )
        )
    late = []
    number = iter(range(len(spans), SLOTS))
    for k, (_, last) in enumerate(spans):
        if carried[k] is not None:
            target = start.at[:, pl.ds(k * rows, rows), :]
            copies.append(pltpu.make_async_copy(carried[k], target, sems.at[next(number)]))
        if last == total:
            late.append(pltpu.make_async_copy(squares[k], square, sems.at[next(number)]))
            for n in range(earlier):
                late.append(
                    pltpu.make_async_copy(before[n].at[0], outs[k].at[n], sems.at[next(number)])
                )
    if keep:
        late.append(pltpu.make_async_copy(tie_ref, same_ref, sems.at[next(number)]))
    for copy in copies + late:
        copy.start()
    zeros = jnp.zeros(wa_ref.shape, jnp.bfloat16)
    for parity in range(2):
        win[parity, pl.ds(0, dim), :] = ws_ref[...] * jnp.bfloat16(0.5)
        win[parity, pl.ds(dim + parity * act_dim, act_dim), :] = wa_ref[...] * jnp.bfloat16(0.5)
        win[parity, pl.ds(dim + (1 - parity) * act_dim, act_dim), :] = zeros
    for k in range(len(spans)):
        for env in range(envs):
            at = pl.ds(k * rows + env * cands, cands)
            if carried[k] is None:
                start[0, at, :] = jnp.broadcast_to(begin_ref[pl.ds(env, 1), :], (cands, dim))
            goal[at, :] = jnp.broadcast_to(goal_ref[pl.ds(env, 1), :], (cands, dim))
        at = pl.ds(k * rows, rows)
        if carried[k] is None:
            start[1, at, :] = jnp.zeros((rows, dim), jnp.float32)
    bias_in = bin_ref[...] * 0.5
    for copy in copies:
        copy.wait()

    many = 4 if steps % 4 == 0 else 2

    def some_steps(k, carry):
        state, error = carry
        for n in range(many):
            parity = n % 2
            at = pl.multiple_of((k * many + n - parity) * act_dim, 2 * act_dim)
            pair = moves[:, pl.ds(at, 2 * act_dim)]
            joined = jnp.concatenate([state.astype(jnp.bfloat16), pair], axis=1)
            half = jnp.dot(joined, win[parity], preferred_element_type=jnp.float32) + bias_in
            hidden = (half + half * jnp.tanh(half)).astype(jnp.bfloat16)
            moved = jnp.dot(hidden, wout_ref[...], preferred_element_type=jnp.float32)
            state = jnp.tanh(state + moved + bout_ref[...])
            gap = state - goal[...]
            error = error + gap * gap
        return state, error

    state, error = lax.fori_loop(0, steps // many, some_steps, (start[0], start[1]))
    for copy in late:
        copy.wait()
    for k, (_, last) in enumerate(spans):
        part = slice(k * rows, (k + 1) * rows)
        if last < total:
            outs[k][0] = state[part]
            outs[k][1] = error[part]
            continue
        both = error[part] / (dim * total) + square[...] * (ACT_COST / (act_dim * total))
        cost = jnp.broadcast_to(jnp.sum(both, axis=1, keepdims=True), (rows, LANES))
        lane = lax.broadcasted_iota(jnp.int32, (cands, LANES), 1)
        table = jnp.zeros((cands, LANES), jnp.float32)
        for env in range(envs):
            table = jnp.where(lane == env, cost[env * cands : (env + 1) * cands], table)
        outs[k][earlier] = table[:, :envs]


def rollout(parts, fixed, before, tie, act_dim, keep):
    rows, width = parts[0][0].shape
    envs, dim = fixed[0].shape
    cands = rows // envs
    total = width // act_dim
    spans = [(p[3], p[4]) for p in parts]
    steps = spans[0][1] - spans[0][0]
    assert all(b - a == steps and a % 2 == 0 for a, b in spans) and steps % 2 == 0
    acts = [p[0] for p in parts]
    carried = [p[2] for p in parts if p[3]]
    squares = [p[1] for p in parts if p[4] == total]
    shapes = [
        (1 + len(before), cands, envs) if last == total else (2, rows, dim) for _, last in spans
    ]
    loose = carried + squares
    assert len(squares) <= 1
    return pl.pallas_call(
        functools.partial(
            rollout_body, spans=spans, act_dim=act_dim, total=total, earlier=len(before), keep=keep
        ),
        grid=(1,),
        in_specs=[HBM] * (len(acts) + len(loose))
        + [VMEM] * len(fixed)
        + [HBM] * (len(before) + 1),
        out_specs=[whole(shape) for shape in shapes] + [VMEM] * keep,
        out_shape=[in_hbm(shape) for shape in shapes]
        + [jax.ShapeDtypeStruct(tie.shape, tie.dtype)] * keep,
        scratch_shapes=[
            pltpu.VMEM((len(parts) * rows, steps * act_dim), jnp.bfloat16),
            pltpu.VMEM((2, dim + 2 * act_dim, fixed[2].shape[1]), jnp.bfloat16),
            pltpu.VMEM((2, len(parts) * rows, dim), jnp.float32),
            pltpu.VMEM((len(parts) * rows, dim), jnp.float32),
            pltpu.VMEM((rows, LANES), jnp.float32),
            pltpu.SemaphoreType.DMA((SLOTS,)),
        ],
        cost_estimate=pl.CostEstimate(flops=ROLL_FLOPS, bytes_accessed=1 << 20, transcendentals=0),
        compiler_params=pltpu.CompilerParams(vmem_limit_bytes=10 << 20),
        name="rollout",
    )(*map(stay, acts), *map(stay, loose), *fixed, *map(stay, before), stay(tie))


def shards(
    white,
    mean_init,
    std_init,
    init_state,
    goal_state,
    w_state,
    w_action,
    w_out,
    bias_in,
    bias_out,
    elite_idx,
):
    iters, envs, cands, flat = white.shape
    act_dim = w_action.shape[0]
    length = flat // act_dim
    width = mean_init.shape[1]
    horizon = width // act_dim
    half = width // 2
    elites = elite_idx.shape[2]
    groups = lax.axis_size("env")
    peers = lax.axis_size("cand")
    lines = 2 * envs
    envs_total = envs * groups
    rows = envs * cands
    assert lines == peers and rows % 16 == 0
    assert iters == 3 and horizon == 40
    mine = lax.axis_index("cand").astype(jnp.int32)[None]
    fixed = (init_state, goal_state, w_state, w_action, w_out, bias_in[None], bias_out[None])
    white = white.reshape(iters, rows, flat)
    elite_idx = jnp.swapaxes(elite_idx, 0, 1)
    mix = functools.partial(lax.all_to_all, axis_name="cand", split_axis=0, concat_axis=0, tiled=True)
    acts, asq, held, costs = {}, {}, {}, {}

    def part(it, first, last):
        return (acts[it], asq[it], held.get(it), first, last)

    def play(parts, tie, before=(), keep=False):
        outs = rollout([part(*p) for p in parts], fixed, before, tie, act_dim, keep)
        for (it, _, last), out in zip(parts, outs):
            if last < horizon:
                held[it] = out
            else:
                costs[it] = out
        return outs[-1] if keep else outs[0]

    (noise,) = noise_of(white, 0, 1, None, act_dim, horizon)
    state, tie = (mean_init, std_init), mine
    for it in range(iters):
        acts[it], asq[it], sums, own = actions_of(
            noise, max(it - 1, 0), elite_idx, mine, tie, state, it, envs_total, lines, half
        )
        parts = mix(sums)
        if it == 0:
            noise, own = noise_of(white, 1, iters - 1, own, act_dim, horizon)
        elif it == 1:
            own = play([(0, 16, 28), (1, 0, 12)], own, keep=True)
        else:
            own = play([(1, 24, horizon), (2, 0, 16)], own, keep=True)
        piece, peak = refit(parts, own, elites, groups)
        peaks = lax.all_to_all(peak, "env", 0, 0, tiled=True)
        tie = mine if it < iters - 1 else play([(2, 16, 20)], peak)
        spread, token = to_all(piece, peaks, tie, lines)
        state = (mix(spread),)
        if it == 0:
            tie = play([(0, 0, 16)], token)
        elif it == 1:
            tie = play([(0, 28, horizon), (1, 12, 24)], token)
        else:
            tie = play([(2, 20, horizon)], token, (costs[0], costs[1]))
    mean, std = finished(state[0], envs, width, envs_total)
    return (mean, std, jnp.swapaxes(costs[iters - 1], 1, 2))


def solution(mesh):
    in_specs = (
        P(None, "env", "cand", None),
        P("env", None),
        P("env", None),
        P("env", None),
        P("env", None),
        P(),
        P(),
        P(),
        P(),
        P(),
        P("env", None, None),
    )
    out_specs = (P("env", None), P("env", None), P(None, "env", "cand"))
    return jax.shard_map(shards, mesh=mesh, in_specs=in_specs, out_specs=out_specs, check_vma=False)
```

```python
import functools

import jax
import jax.numpy as jnp
import numpy as np
from jax import lax
from jax.experimental import pallas as pl
from jax.experimental.pallas import tpu as pltpu
from jax.sharding import PartitionSpec as P

BETA_EXP = 2.5
MOMENTUM = 0.1
FLOOR_SHARE = 0.1
ACT_COST = 0.1
LANES = 128
SLOTS = 8
ROLL_FLOPS = 1 << 28
VMEM = pl.BlockSpec(memory_space=pltpu.VMEM)
SMEM = pl.BlockSpec(memory_space=pltpu.SMEM)
HBM = pl.BlockSpec(memory_space=pltpu.HBM)


def whole(shape):
    return pl.BlockSpec(shape, lambda i: (0,) * len(shape))


def stay(array):
    return pltpu.with_memory_space_constraint(array, pltpu.HBM)


def in_hbm(shape, dtype=jnp.float32):
    return pltpu.HBM(shape, dtype)


def color_kernel(length):
    freqs = np.arange(length // 2 + 1)
    scale = (np.maximum(freqs, 1).astype(np.float32) / np.float32(length)) ** np.float32(-BETA_EXP / 2)
    kernel = np.fft.irfft(scale.astype(np.float64), n=length)
    kernel = kernel / np.sqrt(np.sum(kernel * kernel))
    return np.asarray(kernel, np.float32).astype(jnp.bfloat16).astype(np.float32)


def noise_body(*refs, act_dim, first, keep):
    white_ref, out_ref = refs[0], refs[1 + keep]
    rows_in, packed, fill, sems = refs[-4:]
    count, _, width = out_ref.shape
    flat = white_ref.shape[2]
    length = flat // act_dim
    group = act_dim // 2
    per = 256 // group
    part = length * group

    def fetch(one):
        return pltpu.make_async_copy(white_ref.at[first + one], rows_in.at[one], sems.at[one])

    for one in range(count):
        fetch(one).start()
    if keep:
        hand = pltpu.make_async_copy(refs[1], refs[3], sems.at[count])
        hand.start()
    kernel = color_kernel(length)
    row = lax.broadcasted_iota(jnp.int32, (group, 256), 0)
    hit = lax.broadcasted_iota(jnp.int32, (group, 256), 1) % group == row
    spot = lax.broadcasted_iota(jnp.int32, (1, 256), 1) // group

    def step_at(n):
        return n // 4 * 4 + (0, 2, 1, 3)[n % 4]

    for n in range(length):
        band = jnp.full((1, 256), float(kernel[-step_at(n) % length]), jnp.float32)
        for q in range(1, per):
            band = jnp.where(spot == q, float(kernel[(step_at(q) - step_at(n)) % length]), band)
        tile = jnp.where(hit, band, 0.0).astype(jnp.bfloat16)
        fill[pl.ds(n * group, group), :] = tile
        fill[pl.ds(part + n * group, group), :] = tile
    even = lax.broadcasted_iota(jnp.int32, (1, LANES), 1) // group % 2 == 0

    def swap(a, b):
        low = jnp.where(even, a, pltpu.roll(b, group, 1))
        return low, jnp.where(even, pltpu.roll(a, LANES - group, 1), b)

    for one in range(count):
        fetch(one).wait()
        for k in range(flat // 256):
            pair = [
                rows_in[one, :, pl.ds(k * 256 + side * LANES, LANES)].astype(jnp.float32)
                for side in range(2)
            ]
            for side, piece in enumerate(swap(*pair)):
                packed[side, :, pl.ds(k * LANES, LANES)] = piece.astype(jnp.bfloat16)
        for block in range(width // (per * act_dim)):
            weights = fill[pl.ds((part - block * 256) % part, part), :]
            sides = [
                jnp.dot(packed[side], weights, preferred_element_type=jnp.float32)
                for side in range(2)
            ]
            for h in range(2):
                pair = [side[:, h * LANES : (h + 1) * LANES] for side in sides]
                at = block * 512 + h * 256
                for side, piece in enumerate(swap(*pair)):
                    out_ref[one, :, pl.ds(at + side * LANES, LANES)] = piece
    if keep:
        hand.wait()


def noise_of(white, first, count, own, act_dim, horizon):
    _, rows, flat = white.shape
    width = horizon * act_dim
    keep = own is not None
    assert act_dim == 64 and horizon % 8 == 0
    shapes = [jax.ShapeDtypeStruct((count, rows, width), jnp.float32)]
    if keep:
        shapes.append(jax.ShapeDtypeStruct(own.shape, own.dtype))
    return pl.pallas_call(
        functools.partial(noise_body, act_dim=act_dim, first=first, keep=keep),
        in_specs=[HBM] * (1 + keep),
        out_specs=[VMEM] * (1 + keep),
        out_shape=shapes,
        scratch_shapes=[
            pltpu.VMEM((count, rows, flat), jnp.bfloat16),
            pltpu.VMEM((2, rows, flat // 2), jnp.bfloat16),
            pltpu.VMEM((flat, 256), jnp.bfloat16),
            pltpu.SemaphoreType.DMA((count + 1,)),
        ],
        cost_estimate=pl.CostEstimate(flops=ROLL_FLOPS, bytes_accessed=1 << 20, transcendentals=0),
        compiler_params=pltpu.CompilerParams(vmem_limit_bytes=16 << 20),
        name="noise",
    )(stay(white), *([stay(own)] if keep else []))


def stats_of(state_ref, envs, half, envs_total):
    peaks = state_ref[:, 0, pl.ds(2 * half, LANES)]
    pair = jnp.max(peaks.reshape(envs, 2, LANES), axis=1)
    peak = jnp.max(pair, axis=(0, 1), keepdims=True)
    total = jnp.sum(jnp.sum(pair, axis=0, keepdims=True), axis=1, keepdims=True)
    return FLOOR_SHARE * peak, 0.5 + total / (peak * envs_total)


def action_body(*refs, it, envs_total):
    first = it == 0
    if first:
        noise_ref, elite_ref, mine_ref, tie_ref, mean_ref, std_ref = refs[:6]
    else:
        noise_ref, elite_ref, mine_ref, tie_ref, state_ref = refs[:5]
    acts_out, asq_out, sums_out, own_out, acts_ref, asq_ref, sums_ref, own_ref, sems = refs[-9:]
    half = sums_ref.shape[2]
    rows = acts_ref.shape[0]
    envs = sums_ref.shape[0] // 2
    cands = rows // envs
    me = mine_ref[0]
    if first:
        lanes = pl.ds(pl.multiple_of((me % 2) * half, LANES), half)
        own_ref[0:1, :] = mean_ref[pl.ds(me // 2, 1), lanes]
        own_ref[1:2, :] = std_ref[pl.ds(me // 2, 1), lanes]
    else:
        floor, gain = stats_of(state_ref, envs, half, envs_total)
        own_ref[0:1, :] = state_ref[me, 0:1, pl.ds(0, half)]
        own_ref[1:2, :] = jnp.maximum(state_ref[me, 0:1, pl.ds(half, half)], floor) * gain
    per = 4

    def send(part):
        at = pl.ds(part * per * cands, per * cands)
        pair = pl.ds(part * per * 2, per * 2)
        trio = ((acts_ref, acts_out, at), (asq_ref, asq_out, at), (sums_ref, sums_out, pair))
        return [
            pltpu.make_async_copy(source.at[rows], target.at[rows], sems.at[3 * part + k])
            for k, (source, target, rows) in enumerate(trio)
        ]

    def send_own():
        return pltpu.make_async_copy(own_ref, own_out, sems.at[3 * (envs // per)])

    send_own().start()

    ids = me * cands + lax.broadcasted_iota(jnp.int32, (cands, 1), 0)
    for env in range(envs):
        at = pl.ds(env * cands, cands)
        chosen = elite_ref[it, env : env + 1, :] == ids
        member = jnp.sum(jnp.where(chosen, 1.0, 0.0), axis=1, keepdims=True)
        member = jnp.broadcast_to(member, (cands, LANES))
        square = jnp.zeros((cands, LANES), jnp.float32)
        for side in range(2):
            line = 2 * env + side
            for step in range(half // LANES):
                lanes = pl.ds(step * LANES, LANES)
                whole = pl.ds(side * half + step * LANES, LANES)
                if first:
                    center = mean_ref[pl.ds(env, 1), whole]
                    spread = std_ref[pl.ds(env, 1), whole]
                else:
                    center = state_ref[line, 0:1, lanes]
                    mixed = state_ref[line, 0:1, pl.ds(half + step * LANES, LANES)]
                    spread = jnp.maximum(mixed, floor) * gain
                action = jnp.clip(center + spread * noise_ref[0, at, whole], -1.0, 1.0)
                acts_ref[at, whole] = action.astype(jnp.bfloat16)
                both = action * action
                square = square + both
                sums_ref[line, 0:1, lanes] = jnp.sum(action * member, axis=0, keepdims=True)
                sums_ref[line, 1:2, lanes] = jnp.sum(both * member, axis=0, keepdims=True)
        asq_ref[at, :] = square
        if env % per == per - 1:
            for copy in send(env // per):
                copy.start()
    for part in range(envs // per):
        for copy in send(part):
            copy.wait()
    send_own().wait()


def actions_of(noise, at, elite_idx, mine, tie, state, it, envs_total, lines, half):
    _, rows, width = noise.shape
    return pl.pallas_call(
        functools.partial(action_body, it=it, envs_total=envs_total),
        grid=(1,),
        in_specs=[pl.BlockSpec((1, rows, width), lambda i: (at, 0, 0)), VMEM, SMEM, HBM]
        + [VMEM] * len(state),
        out_specs=[HBM] * 4,
        out_shape=[
            in_hbm((rows, width), jnp.bfloat16),
            in_hbm((rows, LANES)),
            in_hbm((lines, 2, half)),
            in_hbm((2, half)),
        ],
        scratch_shapes=[
            pltpu.VMEM((rows, width), jnp.bfloat16),
            pltpu.VMEM((rows, LANES), jnp.float32),
            pltpu.VMEM((lines, 2, half), jnp.float32),
            pltpu.VMEM((2, half), jnp.float32),
            pltpu.SemaphoreType.DMA((3 * (lines // 8) + 1,)),
        ],
        compiler_params=pltpu.CompilerParams(vmem_limit_bytes=12 << 20),
        name="actions",
    )(noise, elite_idx, mine, stay(tie), *state)


def refit_body(parts_ref, own_ref, slice_ref, peak_ref, *, elites):
    total = jnp.sum(parts_ref[...], axis=0)
    mean = total[0:1] / elites
    variance = jnp.maximum(total[1:2] / elites - mean * mean, 0.0)
    slice_ref[0:1, :] = MOMENTUM * own_ref[0:1, :] + (1.0 - MOMENTUM) * mean
    mixed = MOMENTUM * own_ref[1:2, :] + (1.0 - MOMENTUM) * jnp.sqrt(variance)
    slice_ref[1:2, :] = mixed
    peak_ref[...] = jnp.broadcast_to(jnp.max(mixed, axis=1, keepdims=True)[None], peak_ref.shape)


def refit(parts, own, elites, groups):
    return pl.pallas_call(
        functools.partial(refit_body, elites=elites),
        in_specs=[VMEM, VMEM],
        out_specs=[VMEM, VMEM],
        out_shape=[
            jax.ShapeDtypeStruct(own.shape, jnp.float32),
            jax.ShapeDtypeStruct((groups, 1, LANES), jnp.float32),
        ],
        compiler_params=pltpu.CompilerParams(vmem_limit_bytes=4 << 20),
        name="refit",
    )(parts, own)


def spread_body(slice_ref, peak_ref, tie_ref, out_ref, token_ref):
    lines = out_ref.shape[0]
    half = slice_ref.shape[1]
    lane = lax.broadcasted_iota(jnp.int32, (1, LANES), 1)
    tail = jnp.zeros((1, LANES), jnp.float32)
    for group in range(peak_ref.shape[0]):
        tail = jnp.where(lane == group, peak_ref[group], tail)
    for side in range(2):
        main = jnp.broadcast_to(slice_ref[side : side + 1, :][None], (lines, 1, half))
        out_ref[:, :, pl.ds(side * half, half)] = main
    token_ref[...] = jnp.broadcast_to(tail, token_ref.shape)
    out_ref[:, :, pl.ds(2 * half, LANES)] = jnp.broadcast_to(tail[None], (lines, 1, LANES))


def to_all(piece, peaks, tie, lines):
    half = piece.shape[1]
    return pl.pallas_call(
        spread_body,
        grid=(1,),
        in_specs=[VMEM, VMEM, HBM],
        out_specs=[whole((lines, 1, 2 * half + LANES)), whole((8, LANES))],
        out_shape=[in_hbm((lines, 1, 2 * half + LANES)), in_hbm((8, LANES))],
        compiler_params=pltpu.CompilerParams(vmem_limit_bytes=4 << 20),
        name="to_all",
    )(piece, peaks, stay(tie))


def final_body(state_ref, mean_ref, std_ref, *, envs_total):
    envs, width = mean_ref.shape
    half = width // 2
    floor, gain = stats_of(state_ref, envs, half, envs_total)
    for env in range(envs):
        for side in range(2):
            lanes = pl.ds(side * half, half)
            line = 2 * env + side
            mean_ref[pl.ds(env, 1), lanes] = state_ref[line, 0:1, pl.ds(0, half)]
            std_ref[pl.ds(env, 1), lanes] = (
                jnp.maximum(state_ref[line, 0:1, pl.ds(half, half)], floor) * gain
            )


def finished(state, envs, width, envs_total):
    shape = jax.ShapeDtypeStruct((envs, width), jnp.float32)
    return pl.pallas_call(
        functools.partial(final_body, envs_total=envs_total),
        in_specs=[VMEM],
        out_specs=[VMEM, VMEM],
        out_shape=[shape, shape],
        compiler_params=pltpu.CompilerParams(vmem_limit_bytes=4 << 20),
        name="finished",
    )(state)


def rollout_body(*refs, spans, act_dim, total, earlier, keep):
    refs = list(refs)
    take = lambda n: [refs.pop(0) for _ in range(n)]
    acts = take(len(spans))
    carried = [take(1)[0] if first else None for first, _ in spans]
    squares = [take(1)[0] if last == total else None for _, last in spans]
    begin_ref, goal_ref, ws_ref, wa_ref, wout_ref, bin_ref, bout_ref = take(7)
    before = take(earlier)
    tie_ref = take(1)[0]
    outs = take(len(spans))
    same_ref = take(1)[0] if keep else None
    moves, win, start, goal, square, sems = refs
    envs, dim = begin_ref.shape
    rows = acts[0].shape[0]
    cands = rows // envs
    steps = spans[0][1] - spans[0][0]
    copies = []
    for k, (first, last) in enumerate(spans):
        copies.append(
            pltpu.make_async_copy(
                acts[k].at[:, pl.ds(first * act_dim, steps * act_dim)],
                moves.at[pl.ds(k * rows, rows), :],
                sems.at[k],
            )
        )
    late = []
    number = iter(range(len(spans), SLOTS))
    for k, (_, last) in enumerate(spans):
        if carried[k] is not None:
            target = start.at[:, pl.ds(k * rows, rows), :]
            copies.append(pltpu.make_async_copy(carried[k], target, sems.at[next(number)]))
        if last == total:
            late.append(pltpu.make_async_copy(squares[k], square, sems.at[next(number)]))
            for n in range(earlier):
                late.append(
                    pltpu.make_async_copy(before[n].at[0], outs[k].at[n], sems.at[next(number)])
                )
    if keep:
        late.append(pltpu.make_async_copy(tie_ref, same_ref, sems.at[next(number)]))
    for copy in copies + late:
        copy.start()
    zeros = jnp.zeros(wa_ref.shape, jnp.bfloat16)
    for parity in range(2):
        win[parity, pl.ds(0, dim), :] = ws_ref[...] * jnp.bfloat16(0.5)
        win[parity, pl.ds(dim + parity * act_dim, act_dim), :] = wa_ref[...] * jnp.bfloat16(0.5)
        win[parity, pl.ds(dim + (1 - parity) * act_dim, act_dim), :] = zeros
    for k in range(len(spans)):
        for env in range(envs):
            at = pl.ds(k * rows + env * cands, cands)
            if carried[k] is None:
                start[0, at, :] = jnp.broadcast_to(begin_ref[pl.ds(env, 1), :], (cands, dim))
            goal[at, :] = jnp.broadcast_to(goal_ref[pl.ds(env, 1), :], (cands, dim))
        at = pl.ds(k * rows, rows)
        if carried[k] is None:
            start[1, at, :] = jnp.zeros((rows, dim), jnp.float32)
    bias_in = bin_ref[...] * 0.5
    for copy in copies:
        copy.wait()

    many = 4 if steps % 4 == 0 else 2

    def some_steps(k, carry):
        state, error = carry
        for n in range(many):
            parity = n % 2
            at = pl.multiple_of((k * many + n - parity) * act_dim, 2 * act_dim)
            pair = moves[:, pl.ds(at, 2 * act_dim)]
            joined = jnp.concatenate([state.astype(jnp.bfloat16), pair], axis=1)
            half = jnp.dot(joined, win[parity], preferred_element_type=jnp.float32) + bias_in
            hidden = (half + half * jnp.tanh(half)).astype(jnp.bfloat16)
            moved = jnp.dot(hidden, wout_ref[...], preferred_element_type=jnp.float32)
            state = jnp.tanh(state + moved + bout_ref[...])
            gap = state - goal[...]
            error = error + gap * gap
        return state, error

    state, error = lax.fori_loop(0, steps // many, some_steps, (start[0], start[1]))
    for copy in late:
        copy.wait()
    for k, (_, last) in enumerate(spans):
        part = slice(k * rows, (k + 1) * rows)
        if last < total:
            outs[k][0] = state[part]
            outs[k][1] = error[part]
            continue
        both = error[part] / (dim * total) + square[...] * (ACT_COST / (act_dim * total))
        cost = jnp.broadcast_to(jnp.sum(both, axis=1, keepdims=True), (rows, LANES))
        lane = lax.broadcasted_iota(jnp.int32, (cands, LANES), 1)
        table = jnp.zeros((cands, LANES), jnp.float32)
        for env in range(envs):
            table = jnp.where(lane == env, cost[env * cands : (env + 1) * cands], table)
        outs[k][earlier] = table[:, :envs]


def rollout(parts, fixed, before, tie, act_dim, keep):
    rows, width = parts[0][0].shape
    envs, dim = fixed[0].shape
    cands = rows // envs
    total = width // act_dim
    spans = [(p[3], p[4]) for p in parts]
    steps = spans[0][1] - spans[0][0]
    assert all(b - a == steps and a % 2 == 0 for a, b in spans) and steps % 2 == 0
    acts = [p[0] for p in parts]
    carried = [p[2] for p in parts if p[3]]
    squares = [p[1] for p in parts if p[4] == total]
    shapes = [
        (1 + len(before), cands, envs) if last == total else (2, rows, dim) for _, last in spans
    ]
    loose = carried + squares
    assert len(squares) <= 1
    return pl.pallas_call(
        functools.partial(
            rollout_body, spans=spans, act_dim=act_dim, total=total, earlier=len(before), keep=keep
        ),
        grid=(1,),
        in_specs=[HBM] * (len(acts) + len(loose))
        + [VMEM] * len(fixed)
        + [HBM] * (len(before) + 1),
        out_specs=[whole(shape) for shape in shapes] + [VMEM] * keep,
        out_shape=[in_hbm(shape) for shape in shapes]
        + [jax.ShapeDtypeStruct(tie.shape, tie.dtype)] * keep,
        scratch_shapes=[
            pltpu.VMEM((len(parts) * rows, steps * act_dim), jnp.bfloat16),
            pltpu.VMEM((2, dim + 2 * act_dim, fixed[2].shape[1]), jnp.bfloat16),
            pltpu.VMEM((2, len(parts) * rows, dim), jnp.float32),
            pltpu.VMEM((len(parts) * rows, dim), jnp.float32),
            pltpu.VMEM((rows, LANES), jnp.float32),
            pltpu.SemaphoreType.DMA((SLOTS,)),
        ],
        cost_estimate=pl.CostEstimate(flops=ROLL_FLOPS, bytes_accessed=1 << 20, transcendentals=0),
        compiler_params=pltpu.CompilerParams(vmem_limit_bytes=10 << 20),
        name="rollout",
    )(*map(stay, acts), *map(stay, loose), *fixed, *map(stay, before), stay(tie))


def shards(
    white,
    mean_init,
    std_init,
    init_state,
    goal_state,
    w_state,
    w_action,
    w_out,
    bias_in,
    bias_out,
    elite_idx,
):
    iters, envs, cands, flat = white.shape
    act_dim = w_action.shape[0]
    length = flat // act_dim
    width = mean_init.shape[1]
    horizon = width // act_dim
    half = width // 2
    elites = elite_idx.shape[2]
    groups = lax.axis_size("env")
    peers = lax.axis_size("cand")
    lines = 2 * envs
    envs_total = envs * groups
    rows = envs * cands
    assert lines == peers and rows % 16 == 0
    assert iters == 3 and horizon == 40
    mine = lax.axis_index("cand").astype(jnp.int32)[None]
    fixed = (init_state, goal_state, w_state, w_action, w_out, bias_in[None], bias_out[None])
    white = white.reshape(iters, rows, flat)
    elite_idx = jnp.swapaxes(elite_idx, 0, 1)
    mix = functools.partial(lax.all_to_all, axis_name="cand", split_axis=0, concat_axis=0, tiled=True)
    acts, asq, held, costs = {}, {}, {}, {}

    def part(it, first, last):
        return (acts[it], asq[it], held.get(it), first, last)

    def play(parts, tie, before=(), keep=False):
        outs = rollout([part(*p) for p in parts], fixed, before, tie, act_dim, keep)
        for (it, _, last), out in zip(parts, outs):
            if last < horizon:
                held[it] = out
            else:
                costs[it] = out
        return outs[-1] if keep else outs[0]

    (noise,) = noise_of(white, 0, 1, None, act_dim, horizon)
    state, tie = (mean_init, std_init), mine
    for it in range(iters):
        acts[it], asq[it], sums, own = actions_of(
            noise, max(it - 1, 0), elite_idx, mine, tie, state, it, envs_total, lines, half
        )
        parts = mix(sums)
        if it == 0:
            noise, own = noise_of(white, 1, iters - 1, own, act_dim, horizon)
        elif it == 1:
            own = play([(0, 16, 28), (1, 0, 12)], own, keep=True)
        else:
            own = play([(1, 24, horizon), (2, 0, 16)], own, keep=True)
        piece, peak = refit(parts, own, elites, groups)
        peaks = lax.all_to_all(peak, "env", 0, 0, tiled=True)
        tie = mine if it < iters - 1 else play([(2, 16, 20)], peak)
        spread, token = to_all(piece, peaks, tie, lines)
        state = (mix(spread),)
        if it == 0:
            tie = play([(0, 0, 16)], token)
        elif it == 1:
            tie = play([(0, 28, horizon), (1, 12, 24)], token)
        else:
            tie = play([(2, 20, horizon)], token, (costs[0], costs[1]))
    mean, std = finished(state[0], envs, width, envs_total)
    return (mean, std, jnp.swapaxes(costs[iters - 1], 1, 2))


def solution(mesh):
    in_specs = (
        P(None, "env", "cand", None),
        P("env", None),
        P("env", None),
        P("env", None),
        P("env", None),
        P(),
        P(),
        P(),
        P(),
        P(),
        P("env", None, None),
    )
    out_specs = (P("env", None), P("env", None), P(None, "env", "cand"))
    return jax.shard_map(shards, mesh=mesh, in_specs=in_specs, out_specs=out_specs, check_vma=False)
```
